32 devices in a mesh: seq: 16 (over z, y, core), sub: 2 (over x).
Axes of the slice: x: 2, y: 2, z: 4, core: 2. Of those that a mesh axis runs over, the one named last changes fastest.
Arguments:
- tokens: bfloat16 [4096, 1024], P(('seq', 'sub')), may hold values from -6 to 6
- cotangent: bfloat16 [4096, 1024], P(('seq', 'sub')), may hold values from -6 to 6
- fine_qkv: bfloat16 [1024, 3, 1024], replicated, may hold values from -0.1875 to 0.1875
- fine_out: bfloat16 [1024, 1024], replicated, may hold values from -0.1875 to 0.1875
- coarse_qkv: bfloat16 [1024, 3, 1024], P(None, None, 'sub'), may hold values from -0.1875 to 0.1875
- coarse_out: bfloat16 [1024, 1024], P('sub'), may hold values from -0.5 to 0.5
Outputs:
- output: bfloat16 [4096, 1024], P(('seq', 'sub'))
- grad_tokens: bfloat16 [4096, 1024], P(('seq', 'sub'))
The draws below stay inside these ranges and needn't reach their ends.
All inputs are finite; a program needn't handle non-finite values.
Results may differ from the reference program's by a relative error of at most 0.02.
Values may be sent and summed in bfloat16 or wider, within the bound.
A program may use at most 128 MiB of HBM per device.

```python
import jax
import jax.numpy as jnp
from jax import lax

D = 1024
HEADS = 16
HEAD_DIM = 64
WINDOW = 512
POOL = 16
SEQ_LEN = 4096


def level_of(key, dims, cuts, low, top_value):
    factor_of, own = 1.0, jax.random.fold_in(key, 6)
    for axis_at, parts in cuts:
        steps = jnp.exp(jax.random.uniform(jax.random.fold_in(own, axis_at), (parts,), jnp.float32, low / len(cuts), top_value / len(cuts)))
        factor_of = factor_of * jnp.repeat(steps, dims[axis_at] // parts).reshape([-1 if axis == axis_at else 1 for axis in range(len(dims))])
    return factor_of


def normal_values(key, shape, deviation, bound, shards=(), kind=jnp.bfloat16):
    entries = deviation * jax.random.normal(key, shape, jnp.float32)
    if shards:
        entries = entries * level_of(key, shape, shards, -0.22, 0.18)
    return jnp.clip(entries, -bound, bound).astype(kind)


def setup_inputs(seed: int = 0) -> dict:
    splits = jax.random.split(jax.random.key(seed), 7)
    tokens = normal_values(splits[0], (SEQ_LEN, D), 1.0, 6.0, ((0, 32),))
    cotangent = normal_values(splits[1], (SEQ_LEN, D), 1.0, 6.0, ((0, 32),))
    fine_qkv = normal_values(splits[2], (D, 3, D), D ** -0.5, 0.1875)
    fine_out = normal_values(splits[3], (D, D), D ** -0.5, 0.1875)
    coarse_qkv = normal_values(splits[4], (D, 3, D), D ** -0.5, 0.1875, ((2, 2),))
    coarse_out = normal_values(splits[5], (D, D), (D // 8) ** -0.5, 0.5, ((0, 2),))
    return {"tokens": tokens, "cotangent": cotangent, "fine_qkv": fine_qkv, "fine_out": fine_out, "coarse_qkv": coarse_qkv, "coarse_out": coarse_out}


EPS = 1e-06

def rms_rows(values):
    widened = values.astype(jnp.float32)
    factor = lax.rsqrt(lax.optimization_barrier(jnp.mean(widened * widened, axis=-1, keepdims=True)) + EPS)
    return (widened * factor, factor)

def norm_back(grad_rows, normed, factor):
    return factor * (grad_rows - normed * lax.optimization_barrier(jnp.mean(normed * grad_rows, axis=-1, keepdims=True)))

def project_rows(normed_b, weight):
    row_count = normed_b.shape[0]
    local_width = weight.shape[2]
    projected = jnp.dot(normed_b, weight.reshape(weight.shape[0], 3 * local_width), preferred_element_type=jnp.float32)
    projected = projected.reshape(row_count, 3, local_width // HEAD_DIM, HEAD_DIM)
    query_unit, query_scale = rms_rows(projected[:, 0])
    key_unit, key_scale = rms_rows(projected[:, 1])
    return (query_unit, query_scale, key_unit, key_scale, projected[:, 2])

def fdot(spec, left, right):
    return jnp.einsum(spec, left.astype(jnp.float32), right.astype(jnp.float32), precision=lax.Precision.HIGHEST)

def window_exp(query_blk, key_blk, first_pos):
    scores = fdot('qhd,khd->hqk', query_blk, key_blk) * HEAD_DIM ** (-0.5)
    query_pos = lax.broadcasted_iota(jnp.int32, (query_blk.shape[0], key_blk.shape[0]), 0)
    key_pos = lax.broadcasted_iota(jnp.int32, (query_blk.shape[0], key_blk.shape[0]), 1)
    gap = WINDOW + query_pos - key_pos
    allowed = (gap >= 0) & (gap < WINDOW) & (first_pos - WINDOW + key_pos >= 0)
    return jnp.where(allowed[None], jnp.exp(scores), 0.0)

def padded_front(rows):
    return jnp.concatenate([jnp.zeros((WINDOW,) + rows.shape[1:], rows.dtype), rows])

def window_forward(queries, key_rows, value_rows):
    total_len = queries.shape[0]
    key_pad = padded_front(key_rows)
    value_pad = padded_front(value_rows)

    def one_block(block_index):
        first_pos = block_index * WINDOW
        query_blk = lax.dynamic_slice_in_dim(queries, first_pos, WINDOW)
        key_blk = lax.dynamic_slice_in_dim(key_pad, first_pos, 2 * WINDOW)
        value_blk = lax.dynamic_slice_in_dim(value_pad, first_pos, 2 * WINDOW)
        numer = window_exp(query_blk, key_blk, first_pos)
        totals = lax.optimization_barrier(jnp.sum(numer, axis=-1))
        probs_half = (numer / totals[:, :, None]).astype(jnp.bfloat16)
        attended = fdot('hqk,khd->qhd', probs_half, value_blk).astype(jnp.bfloat16)
        return (attended, totals)
    attended, totals = lax.map(one_block, jnp.arange(total_len // WINDOW, dtype=jnp.int32))
    return (attended.reshape(queries.shape), totals)

def window_query_grads(queries, key_rows, value_rows, grad_out, totals, deltas):
    total_len = queries.shape[0]
    key_pad = padded_front(key_rows)
    value_pad = padded_front(value_rows)

    def one_block(inputs):
        block_index, block_totals = inputs
        first_pos = block_index * WINDOW
        query_blk = lax.dynamic_slice_in_dim(queries, first_pos, WINDOW)
        key_blk = lax.dynamic_slice_in_dim(key_pad, first_pos, 2 * WINDOW)
        value_blk = lax.dynamic_slice_in_dim(value_pad, first_pos, 2 * WINDOW)
        grad_blk = lax.dynamic_slice_in_dim(grad_out, first_pos, WINDOW)
        delta_blk = lax.dynamic_slice_in_dim(deltas, first_pos, WINDOW)
        probs_full = window_exp(query_blk, key_blk, first_pos) / block_totals[:, :, None]
        prob_grad = fdot('qhd,khd->hqk', grad_blk, value_blk)
        dscore = (probs_full * (prob_grad - delta_blk.T[:, :, None])).astype(jnp.bfloat16)
        return fdot('hqk,khd->qhd', dscore, key_blk) * HEAD_DIM ** (-0.5)
    grads = lax.map(one_block, (jnp.arange(total_len // WINDOW, dtype=jnp.int32), totals))
    return grads.reshape(queries.shape)

def window_key_grads(queries, key_rows, value_rows, grad_out, totals_rows, deltas):
    total_len = queries.shape[0]
    query_pad = jnp.concatenate([queries, jnp.zeros((WINDOW,) + queries.shape[1:], queries.dtype)])
    grad_pad = jnp.concatenate([grad_out, jnp.zeros((WINDOW,) + grad_out.shape[1:], grad_out.dtype)])
    total_pad = jnp.concatenate([totals_rows, jnp.ones((WINDOW, totals_rows.shape[1]), jnp.float32)])
    delta_pad = jnp.concatenate([deltas, jnp.zeros((WINDOW, deltas.shape[1]), jnp.float32)])

    def one_block(block_index):
        first_key = block_index * WINDOW
        key_blk = lax.dynamic_slice_in_dim(key_rows, first_key, WINDOW)
        value_blk = lax.dynamic_slice_in_dim(value_rows, first_key, WINDOW)
        query_blk = lax.dynamic_slice_in_dim(query_pad, first_key, 2 * WINDOW)
        grad_blk = lax.dynamic_slice_in_dim(grad_pad, first_key, 2 * WINDOW)
        total_blk = lax.dynamic_slice_in_dim(total_pad, first_key, 2 * WINDOW)
        delta_blk = lax.dynamic_slice_in_dim(delta_pad, first_key, 2 * WINDOW)
        scores = fdot('qhd,khd->hqk', query_blk, key_blk) * HEAD_DIM ** (-0.5)
        query_pos = lax.broadcasted_iota(jnp.int32, (2 * WINDOW, WINDOW), 0)
        key_pos = lax.broadcasted_iota(jnp.int32, (2 * WINDOW, WINDOW), 1)
        gap = query_pos - key_pos
        allowed = (gap >= 0) & (gap < WINDOW) & (first_key + query_pos < total_len)
        numer = jnp.where(allowed[None], jnp.exp(scores), 0.0)
        probs_full = numer / total_blk.T[:, :, None]
        probs_half = probs_full.astype(jnp.bfloat16)
        prob_grad = fdot('qhd,khd->hqk', grad_blk, value_blk)
        dscore = (probs_full * (prob_grad - delta_blk.T[:, :, None])).astype(jnp.bfloat16)
        key_grad = fdot('hqk,qhd->khd', dscore, query_blk) * HEAD_DIM ** (-0.5)
        value_grad = fdot('hqk,qhd->khd', probs_half, grad_blk)
        return (key_grad, value_grad)
    key_grad, value_grad = lax.map(one_block, jnp.arange(total_len // WINDOW, dtype=jnp.int32))
    return (key_grad.reshape(key_rows.shape), value_grad.reshape(value_rows.shape))

def coarse_head(head_inputs):
    queries, key_rows, value_rows = head_inputs
    length = queries.shape[0]
    scores = jnp.dot(queries, key_rows.T, preferred_element_type=jnp.float32) * HEAD_DIM ** (-0.5)
    query_pos = lax.broadcasted_iota(jnp.int32, (length, length), 0)
    key_pos = lax.broadcasted_iota(jnp.int32, (length, length), 1)
    numer = jnp.where(key_pos <= query_pos, jnp.exp(scores), 0.0)
    totals = lax.optimization_barrier(jnp.sum(numer, axis=-1))
    probs_half = (numer / totals[:, None]).astype(jnp.bfloat16)
    attended = jnp.dot(probs_half, value_rows, preferred_element_type=jnp.float32).astype(jnp.bfloat16)
    return (attended, totals)

def coarse_head_back(head_inputs):
    queries, key_rows, value_rows, attended, grad_out, totals = head_inputs
    length = queries.shape[0]
    scores = jnp.dot(queries, key_rows.T, preferred_element_type=jnp.float32) * HEAD_DIM ** (-0.5)
    query_pos = lax.broadcasted_iota(jnp.int32, (length, length), 0)
    key_pos = lax.broadcasted_iota(jnp.int32, (length, length), 1)
    numer = jnp.where(key_pos <= query_pos, jnp.exp(scores), 0.0)
    probs_full = numer / totals[:, None]
    probs_half = probs_full.astype(jnp.bfloat16)
    deltas = lax.optimization_barrier(jnp.sum(grad_out.astype(jnp.float32) * attended.astype(jnp.float32), axis=-1))
    prob_grad = jnp.dot(grad_out, value_rows.T, preferred_element_type=jnp.float32)
    dscore = (probs_full * (prob_grad - deltas[:, None])).astype(jnp.bfloat16)
    query_grad = jnp.dot(dscore, key_rows, preferred_element_type=jnp.float32) * HEAD_DIM ** (-0.5)
    key_grad = jnp.dot(dscore.T, queries, preferred_element_type=jnp.float32) * HEAD_DIM ** (-0.5)
    value_grad = jnp.dot(probs_half.T, grad_out, preferred_element_type=jnp.float32)
    return (query_grad, key_grad, value_grad)

def contract_last(left, right):
    return lax.dot_general(left, right, (((1,), (1,)), ((), ())), preferred_element_type=jnp.float32)

def reference(tokens, cotangent, fine_qkv, fine_out, coarse_qkv, coarse_out):
    total_len = tokens.shape[0]
    lead_rows = POOL - 1
    coarse_len = total_len // POOL
    normed_fine, scale_fine = rms_rows(tokens)
    query_unit1, query_scale1, key_unit1, key_scale1, value_raw1 = project_rows(normed_fine.astype(jnp.bfloat16), fine_qkv)
    query_one = query_unit1.astype(jnp.bfloat16)
    key_one = key_unit1.astype(jnp.bfloat16)
    value_one = value_raw1.astype(jnp.bfloat16)
    attended_one, totals_one = window_forward(query_one, key_one, value_one)
    hidden = (tokens.astype(jnp.float32) + jnp.dot(attended_one.reshape(total_len, D), fine_out, preferred_element_type=jnp.float32)).astype(jnp.bfloat16)
    shifted = jnp.concatenate([jnp.zeros((lead_rows, D), jnp.bfloat16), hidden[:total_len - lead_rows]])
    pooled = shifted.reshape(coarse_len, POOL, D).astype(jnp.float32).mean(axis=1).astype(jnp.bfloat16)
    normed_coarse, scale_coarse = rms_rows(pooled)
    query_unit2, query_scale2, key_unit2, key_scale2, value_raw2 = project_rows(normed_coarse.astype(jnp.bfloat16), coarse_qkv)
    query_two = jnp.transpose(query_unit2.astype(jnp.bfloat16), (1, 0, 2))
    key_two = jnp.transpose(key_unit2.astype(jnp.bfloat16), (1, 0, 2))
    value_two = jnp.transpose(value_raw2.astype(jnp.bfloat16), (1, 0, 2))
    attended_two, totals_two = lax.map(coarse_head, (query_two, key_two, value_two))
    attended_rows = jnp.transpose(attended_two, (1, 0, 2)).reshape(coarse_len, D)
    coarse_state = (pooled.astype(jnp.float32) + jnp.dot(attended_rows, coarse_out, preferred_element_type=jnp.float32)).astype(jnp.bfloat16)
    output = (hidden.astype(jnp.float32) + jnp.repeat(coarse_state, POOL, axis=0).astype(jnp.float32)).astype(jnp.bfloat16)
    grad_rows = cotangent.astype(jnp.float32)
    coarse_grad = grad_rows.reshape(coarse_len, POOL, D).sum(axis=1)
    grad_att2 = contract_last(coarse_grad.astype(jnp.bfloat16), coarse_out).astype(jnp.bfloat16)
    grad_att2 = jnp.transpose(grad_att2.reshape(coarse_len, HEADS, HEAD_DIM), (1, 0, 2))
    query_grad2, key_grad2, value_grad2 = lax.map(coarse_head_back, (query_two, key_two, value_two, attended_two, grad_att2, totals_two))
    query_grad2 = norm_back(jnp.transpose(query_grad2, (1, 0, 2)), query_unit2, query_scale2)
    key_grad2 = norm_back(jnp.transpose(key_grad2, (1, 0, 2)), key_unit2, key_scale2)
    value_grad2 = jnp.transpose(value_grad2, (1, 0, 2))
    qkv_grad2 = jnp.stack([query_grad2, key_grad2, value_grad2], axis=1).astype(jnp.bfloat16).reshape(coarse_len, 3 * D)
    normed_grad2 = contract_last(qkv_grad2, coarse_qkv.reshape(D, 3 * D))
    pooled_grad = coarse_grad + norm_back(normed_grad2, normed_coarse, scale_coarse)
    spread = jnp.repeat(pooled_grad / POOL, POOL, axis=0)
    hidden_grad = grad_rows + jnp.concatenate([spread[lead_rows:], jnp.zeros((lead_rows, D), jnp.float32)])
    grad_att1 = contract_last(hidden_grad.astype(jnp.bfloat16), fine_out).astype(jnp.bfloat16).reshape(total_len, HEADS, HEAD_DIM)
    deltas_one = lax.optimization_barrier(jnp.sum(grad_att1.astype(jnp.float32) * attended_one.astype(jnp.float32), axis=-1))
    totals_rows = jnp.transpose(totals_one, (0, 2, 1)).reshape(total_len, HEADS)
    query_grad1 = window_query_grads(query_one, key_one, value_one, grad_att1, totals_one, deltas_one)
    key_grad1, value_grad1 = window_key_grads(query_one, key_one, value_one, grad_att1, totals_rows, deltas_one)
    query_grad1 = norm_back(query_grad1, query_unit1, query_scale1)
    key_grad1 = norm_back(key_grad1, key_unit1, key_scale1)
    qkv_grad1 = jnp.stack([query_grad1, key_grad1, value_grad1], axis=1).astype(jnp.bfloat16).reshape(total_len, 3 * D)
    normed_grad1 = contract_last(qkv_grad1, fine_qkv.reshape(D, 3 * D))
    grad_tokens = (hidden_grad + norm_back(normed_grad1, normed_fine, scale_fine)).astype(jnp.bfloat16)
    return (output, grad_tokens)
```

```python
import functools

import jax
import jax.numpy as jnp
from jax import lax
from jax.experimental import pallas as pl
from jax.experimental.pallas import tpu as pltpu
from jax.sharding import PartitionSpec as P

D = 1024
HEADS = 16
HEAD_DIM = 64
WINDOW = 512
POOL = 16
EPS = 1e-06
F32 = jnp.float32
BF16 = jnp.bfloat16
MESH = pl.DeviceIdType.MESH
PAIR = 2 * HEAD_DIM
SCALE = HEAD_DIM ** (-0.5)
VMEM = pl.BlockSpec(memory_space=pltpu.VMEM)
ANY = pl.BlockSpec(memory_space=pl.ANY)
SMEM = pl.BlockSpec(memory_space=pltpu.SMEM)


def dot(a, b):
    return jnp.dot(a, b, preferred_element_type=F32)


def dot_nt(a, b):
    return lax.dot_general(a, b, (((1,), (1,)), ((), ())), preferred_element_type=F32)


def dot_tn(a, b):
    return lax.dot_general(a, b, (((0,), (0,)), ((), ())), preferred_element_type=F32)


def split(x):
    hi = x.astype(BF16)
    return hi, (x - hi.astype(F32)).astype(BF16)


def iota(shape, axis):
    return lax.broadcasted_iota(jnp.int32, shape, axis)


def head_sum(x):
    group = (iota((x.shape[1], 128), 0) // HEAD_DIM == iota((x.shape[1], 128), 1)).astype(F32).astype(BF16)
    hi, lo = split(x)
    return dot(hi, group) + dot(lo, group)


def head_spread(f, width):
    group = (iota((128, width), 1) // HEAD_DIM == iota((128, width), 0)).astype(F32).astype(BF16)
    hi, lo = split(f)
    return dot(hi, group) + dot(lo, group)


def head_rms(raw):
    factor = lax.rsqrt(head_sum(raw * raw) / HEAD_DIM + EPS)
    factor = head_spread(factor, raw.shape[1])
    return raw * factor, factor


def head_back(grad, unit, factor):
    return factor * (grad - unit * head_spread(head_sum(unit * grad) / HEAD_DIM, grad.shape[1]))


def rms_rows(x):
    factor = lax.rsqrt(jnp.mean(x * x, axis=-1, keepdims=True) + EPS)
    return x * factor, factor


def row_back(grad, normed, factor):
    return factor * (grad - normed * jnp.mean(normed * grad, axis=-1, keepdims=True))


def both(pair):
    low = iota(pair.shape, 1) < HEAD_DIM
    wide = pair.astype(F32)
    return jnp.concatenate([jnp.where(low, wide, 0.0), jnp.where(low, 0.0, wide)]).astype(BF16)


def pick(stacked):
    half = stacked.shape[0] // 2
    low = iota((half, PAIR), 1) < HEAD_DIM
    return jnp.where(low, stacked[:half], stacked[half:])


def place():
    subs = lax.axis_size("sub")
    count = lax.axis_size("seq") * subs
    me = lax.axis_index("seq") * subs + lax.axis_index("sub")
    return me, count, subs


def coords(index, subs):
    return (index // subs, index % subs)


def greet_all():
    me, count, subs = place()
    barrier = pltpu.get_barrier_semaphore()

    @pl.loop(1, count)
    def _(k):
        pl.semaphore_signal(
            barrier, inc=1, device_id=coords((me + k) % count, subs), device_id_type=MESH
        )

    pl.semaphore_wait(barrier, count - 1)


def remote(src, dst, send, recv, target, subs):
    return pltpu.make_async_remote_copy(
        src_ref=src, dst_ref=dst, send_sem=send, recv_sem=recv,
        device_id=coords(target, subs), device_id_type=MESH,
    )


class Spread:
    def __init__(self, src, dst, sends, recvs, local):
        self.me, self.count, self.subs = place()
        self.args = (src, dst, sends, recvs, local)

    def copy(self, k):
        src, dst, sends, recvs, _ = self.args
        target = (self.me + k) % self.count
        return remote(src, dst.at[self.me], sends.at[k], recvs.at[k], target, self.subs)

    def start(self):
        src, dst, _, _, local = self.args

        @pl.loop(1, self.count)
        def _(k):
            self.copy(k).start()

        pltpu.make_async_copy(src, dst.at[self.me], local).start()

    def wait(self):
        src, dst, sends, recvs, local = self.args

        @pl.loop(1, self.count)
        def _(k):
            self.copy(k).wait_send()
            came = (self.me + self.count - k) % self.count
            remote(src, dst.at[came], sends.at[k], recvs.at[k], came, self.subs).wait_recv()

        pltpu.make_async_copy(src, dst.at[self.me], local).wait()


class Shift:
    def __init__(self, src, dst, send, recv, distance):
        me, count, subs = place()
        self.me, self.subs, self.target = me, subs, me + distance
        self.args = (src, dst, send, recv)
        self.sends = (me + distance >= 0) & (me + distance < count)
        self.gets = (me - distance >= 0) & (me - distance < count)
        self.copy = remote(src, dst, send, recv, jnp.clip(me + distance, 0, count - 1), subs)

    def start(self):
        @pl.when(self.sends)
        def _():
            self.copy.start()

    def wait(self):
        @pl.when(self.sends)
        def _():
            self.copy.wait_send()

        @pl.when(self.gets)
        def _():
            self.copy.wait_recv()


def comm(body, outs, scratch, ident, specs, *args):
    return pl.pallas_call(
        body,
        out_shape=outs,
        in_specs=specs,
        out_specs=jax.tree.map(lambda _: ANY, outs),
        scratch_shapes=scratch,
        compiler_params=pltpu.CompilerParams(collective_id=ident, has_side_effects=True),
    )(*args)


def local_call(body, outs, *args, smem=True):
    return pl.pallas_call(
        body,
        out_shape=outs,
        in_specs=[SMEM] + [VMEM] * (len(args) - 1),
        out_specs=jax.tree.map(lambda _: VMEM, outs),
        compiler_params=pltpu.CompilerParams(vmem_limit_bytes=60 * 1024 * 1024),
    )(*args)


def first_exchange(hops, x_ref, cg_ref, before, after, cg_all, sends, recvs, ag_send, ag_recv, local):
    greet_all()
    spread = Spread(cg_ref, cg_all, ag_send, ag_recv, local)
    moves = []
    for d in range(1, hops + 1):
        moves.append(Shift(x_ref, before.at[hops - d], sends.at[d - 1], recvs.at[d - 1], d))
        moves.append(
            Shift(x_ref, after.at[d - 1], sends.at[hops + d - 1], recvs.at[hops + d - 1], -d)
        )
    for move in moves:
        move.start()
    spread.start()
    for move in moves:
        move.wait()
    spread.wait()


def second_exchange(
    hops, hidden_ref, cot_ref, pooled_all, cot_after, tail, pooled, sends, recvs, ag_send, ag_recv, local
):
    me, count, subs = place()
    rows = hidden_ref.shape[0]
    outs = rows // POOL
    greet_all()
    carry = Shift(hidden_ref.at[pl.ds(rows - POOL, POOL)], tail, sends.at[hops], recvs.at[hops], 1)
    carry.start()
    back = iota((outs, rows), 0) * POOL - iota((outs, rows), 1)
    part = dot(((back >= 0) & (back < POOL)).astype(F32).astype(BF16), hidden_ref[...])
    carry.wait()
    lead = (iota((outs, POOL), 0) == 0) & (iota((outs, POOL), 1) > 0)
    tail_rows = jnp.where(me > 0, tail[...].astype(F32), 0.0).astype(BF16)
    part = part + dot(lead.astype(F32).astype(BF16), tail_rows)
    pooled[...] = (part / POOL).astype(BF16)
    spread = Spread(pooled, pooled_all, ag_send, ag_recv, local)
    spread.start()
    moves = [
        Shift(cot_ref, cot_after.at[d - 1], sends.at[d - 1], recvs.at[d - 1], -d)
        for d in range(1, hops + 1)
    ]
    for move in moves:
        move.start()
    spread.wait()
    for move in moves:
        move.wait()


def third_exchange(far, mixed_all, grad_all, mixed_in, grad_in, sends, recvs, local):
    me, count, subs = place()
    mine = lax.axis_index("sub")
    seq = lax.axis_index("seq")
    outs = mixed_in.shape[1]
    barrier = pltpu.get_barrier_semaphore()
    for k in range(1, subs):
        pl.semaphore_signal(
            barrier, inc=1, device_id=(seq, (mine + k) % subs), device_id_type=MESH
        )
    pl.semaphore_wait(barrier, subs - 1)
    copies = []
    for k in range(1, subs):
        target = seq * subs + (mine + k) % subs
        start = pl.multiple_of(target * outs, outs)
        pieces = (
            (mixed_all.at[pl.ds(start, outs)], mixed_in.at[k]),
            (grad_all.at[pl.ds(start, far)], grad_in.at[k]),
        )
        for which, (src, dst) in enumerate(pieces):
            copies.append(remote(src, dst, sends.at[2 * k + which], recvs.at[2 * k + which], target, subs))
    for copy in copies:
        copy.start()
    start = pl.multiple_of(me * outs, outs)
    own = [
        pltpu.make_async_copy(mixed_all.at[pl.ds(start, outs)], mixed_in.at[0], local.at[0]),
        pltpu.make_async_copy(grad_all.at[pl.ds(start, far)], grad_in.at[0], local.at[1]),
    ]
    for copy in own:
        copy.start()
    for copy in copies + own:
        copy.wait()


def fourth_exchange(hops, stats_ref, after, sends, recvs):
    me, count, subs = place()
    barrier = pltpu.get_barrier_semaphore()
    for d in range(1, hops + 1):
        for other in (me - d, me + d):

            @pl.when((other >= 0) & (other < count))
            def _():
                pl.semaphore_signal(
                    barrier, inc=1, device_id=coords(jnp.clip(other, 0, count - 1), subs),
                    device_id_type=MESH,
                )

    pl.semaphore_wait(barrier, jnp.minimum(me, hops) + jnp.minimum(count - 1 - me, hops))

    moves = [
        Shift(stats_ref, after.at[d - 1], sends.at[d - 1], recvs.at[d - 1], -d)
        for d in range(1, hops + 1)
    ]
    for move in moves:
        move.start()
    for move in moves:
        move.wait()


def window_mask(rows, keys, anchor):
    gap = keys - rows + iota((rows, keys), 0) - iota((rows, keys), 1)
    return (gap >= 0) & (gap < WINDOW) & (anchor - (keys - rows) + iota((rows, keys), 1) >= 0)


def fine_forward(
    pos, before, x_ref, after, w_ref, out_w,
    q_all, k_all, v_all, unit_q, unit_k, scale_q, scale_k, tot_ref, att_ref, hidden_ref,
):
    rows = x_ref.shape[0]
    margin = before.shape[0]
    anchor = pos[0] * rows
    own = x_ref[...].astype(F32)
    prev = before[...].astype(F32)
    prev = jnp.where(anchor - margin + iota(prev.shape, 0) >= 0, prev, 0.0)
    nxt = after[...].astype(F32)
    nxt = jnp.where(anchor + rows + iota(nxt.shape, 0) < pos[1] * rows, nxt, 0.0)
    own_b = rms_rows(own)[0].astype(BF16)
    past_b = jnp.concatenate([rms_rows(prev)[0].astype(BF16), own_b])
    next_b = jnp.concatenate([own_b, rms_rows(nxt)[0].astype(BF16)])
    unit, factor = head_rms(dot(next_b, w_ref[0]))
    q_all[...] = unit.astype(BF16)
    unit_q[...] = unit[:rows]
    scale_q[...] = factor[:rows]
    unit, factor = head_rms(dot(past_b, w_ref[1]))
    k_all[...] = unit.astype(BF16)
    unit_k[...] = unit[margin:]
    scale_k[...] = factor[margin:]
    v_all[...] = dot(past_b, w_ref[2]).astype(BF16)
    mask = window_mask(rows, margin + rows, anchor)
    mask = jnp.concatenate([mask.astype(F32)] * 2) > 0
    lane = iota((rows, 128), 1)
    totals = jnp.ones((rows, 128), F32)
    for p in range(HEADS // 2):
        cols = pl.ds(p * PAIR, PAIR)
        s = dot_nt(both(q_all[pl.ds(0, rows), cols]), k_all[:, cols]) * SCALE
        e = jnp.where(mask, jnp.exp(s), 0.0)
        t = jnp.sum(e, axis=-1, keepdims=True)
        prob = (e * (1.0 / t)).astype(BF16)
        att_ref[:, cols] = pick(dot(prob, v_all[:, cols])).astype(BF16)
        totals = jnp.where(lane == 2 * p, t[:rows], totals)
        totals = jnp.where(lane == 2 * p + 1, t[rows:], totals)
    tot_ref[...] = totals
    hidden_ref[...] = (own + dot(att_ref[...], out_w[...])).astype(BF16)


def coarse_level(pos, pooled_ref, cg_ref, w_ref, out_w, mixed_ref, grad_ref):
    count, width = pooled_ref.shape[0], w_ref.shape[2]
    normed_b = rms_rows(pooled_ref[...].astype(F32))[0].astype(BF16)
    uq, fq = head_rms(dot(normed_b, w_ref[0]))
    uk, fk = head_rms(dot(normed_b, w_ref[1]))
    qb, kb = uq.astype(BF16), uk.astype(BF16)
    vb = dot(normed_b, w_ref[2]).astype(BF16)
    gb = dot_nt(cg_ref[...], out_w[...]).astype(BF16)
    block = min(count, 256)
    att_p, dq_p, dk_p, dv_p = [], [], [], []
    for p in range(width // PAIR):
        cols = slice(p * PAIR, (p + 1) * PAIR)
        att_b, dq_b, dk, dv = [], [], None, None
        kp, vp = kb[:, cols], vb[:, cols]
        for b in range(count // block):
            rows = slice(b * block, (b + 1) * block)
            qs, gs = both(qb[rows, cols]), both(gb[rows, cols])
            s = dot_nt(qs, kp) * SCALE
            where = iota((2 * block, count), 0) % block + b * block >= iota((2 * block, count), 1)
            e = jnp.where(where, jnp.exp(s), 0.0)
            full = e * (1.0 / jnp.sum(e, axis=-1, keepdims=True))
            prob = full.astype(BF16)
            att = pick(dot(prob, vp)).astype(BF16)
            att_b.append(att)
            att2 = jnp.concatenate([att.astype(F32)] * 2)
            delta = jnp.sum(gs.astype(F32) * att2, axis=-1, keepdims=True)
            ds = (full * (dot_nt(gs, vp) - delta)).astype(BF16)
            dq_b.append(pick(dot(ds, kp)) * SCALE)
            dk_t, dv_t = dot_tn(ds, qs) * SCALE, dot_tn(prob, gs)
            dk = dk_t if dk is None else dk + dk_t
            dv = dv_t if dv is None else dv + dv_t
        att_p.append(jnp.concatenate(att_b))
        dq_p.append(jnp.concatenate(dq_b))
        dk_p.append(dk)
        dv_p.append(dv)
    join = lambda parts: jnp.concatenate(parts, axis=1)
    mixed_ref[...] = dot(join(att_p), out_w[...]).astype(BF16)
    dq = head_back(join(dq_p), uq, fq).astype(BF16)
    dk = head_back(join(dk_p), uk, fk).astype(BF16)
    dv = join(dv_p).astype(BF16)
    total = dot_nt(dq, w_ref[0]) + dot_nt(dk, w_ref[1]) + dot_nt(dv, w_ref[2])
    grad_ref[pl.ds(0, count), :] = total.astype(BF16)
    extra = grad_ref.shape[0] - count
    grad_ref[pl.ds(count, extra), :] = jnp.zeros((extra, D), BF16)


def middle(
    pos, hidden_ref, mixed_in, grad_in, pooled_ref, cg_ref, cot_ref, cot_after, att_ref, tot_ref, out_w,
    output_ref, hg_ref, g_all, delta_ref, stats_ref,
):
    rows = hidden_ref.shape[0]
    outs = rows // POOL
    ahead = cot_after.shape[0]
    far = grad_in.shape[1]
    start = pos[0] * rows
    pooled = pooled_ref[...].astype(F32)
    mixed = jnp.sum(mixed_in[...].astype(F32), axis=0)
    state = (pooled[:outs] + mixed).astype(BF16)
    onto = (iota((rows, outs), 0) // POOL == iota((rows, outs), 1)).astype(F32).astype(BF16)
    output_ref[...] = (hidden_ref[...].astype(F32) + dot(onto, state)).astype(BF16)
    nxt = cot_after[...].astype(F32)
    nxt = jnp.where(start + rows + iota(nxt.shape, 0) < pos[1] * rows, nxt, 0.0)
    cot = jnp.concatenate([cot_ref[...].astype(F32), nxt])
    length = rows + ahead
    near = length // POOL
    groups = (iota((near, length), 1) // POOL == iota((near, length), 0)).astype(F32).astype(BF16)
    cg = jnp.concatenate([dot(groups, cot.astype(BF16)), cg_ref[...].astype(F32)[near:]])
    ng = jnp.sum(grad_in[...].astype(F32), axis=0)
    normed, factor = rms_rows(pooled)
    pg = (cg + row_back(ng, normed, factor)) / POOL
    pg = jnp.where(pos[0] * outs + iota(pg.shape, 0) < pos[1] * outs, pg, 0.0)
    lift = ((iota((length, far), 0) + POOL - 1) // POOL == iota((length, far), 1)).astype(F32).astype(BF16)
    hi, lo = split(pg)
    hidden_grad = cot + dot(lift, hi) + dot(lift, lo)
    hg_ref[...] = hidden_grad[:rows]
    g_all[...] = dot_nt(hidden_grad.astype(BF16), out_w[...]).astype(BF16)
    delta = head_sum(g_all[pl.ds(0, rows), :].astype(F32) * att_ref[...].astype(F32))
    delta_ref[...] = delta
    stats_ref[pl.ds(0, HEADS), :] = tot_ref[...].T[:HEADS]
    stats_ref[pl.ds(HEADS, HEADS), :] = delta.T[:HEADS]


def fine_backward(
    pos, x_ref, w_ref, q_all, k_all, v_all, g_all, own_stats, after, tot_ref, delta_ref,
    unit_q, unit_k, scale_q, scale_k, hg_ref, grad_ref,
):
    rows = x_ref.shape[0]
    hops = after.shape[0]
    margin = k_all.shape[0] - rows
    length = q_all.shape[0]
    anchor = pos[0] * rows
    mask = window_mask(rows, margin + rows, anchor)
    mask = jnp.concatenate([mask.astype(F32)] * 2) > 0
    gap = iota((rows, length), 1) - iota((rows, length), 0)
    mask_t = (gap >= 0) & (gap < WINDOW) & (anchor + iota((rows, length), 1) < pos[1] * rows)
    stats = jnp.concatenate([own_stats[...]] + [after[d] for d in range(hops)], axis=1)
    stats = jnp.where(anchor + iota(stats.shape, 1) < pos[1] * rows, stats, 1.0)
    totals, deltas = tot_ref[...], delta_ref[...]
    dq_p, dk_p, dv_p = [], [], []
    for p in range(HEADS // 2):
        cols = pl.ds(p * PAIR, PAIR)
        kp, vp, qp, gp = k_all[:, cols], v_all[:, cols], q_all[:, cols], g_all[:, cols]
        s = dot_nt(both(qp[:rows]), kp) * SCALE
        e = jnp.where(mask, jnp.exp(s), 0.0)
        column = lambda m: jnp.concatenate([m[:, 2 * p : 2 * p + 1], m[:, 2 * p + 1 : 2 * p + 2]])
        ds = e * (1.0 / column(totals)) * (dot_nt(both(gp[:rows]), vp) - column(deltas))
        dq_p.append(pick(dot(ds.astype(BF16), kp)) * SCALE)
        k_own, v_own = kp[margin:], vp[margin:]
        qs, gs = both(qp), both(gp)
        dk = dv = jnp.zeros((rows, PAIR), F32)
        for h in range(2):
            part = slice(h * length, (h + 1) * length)
            st = dot_nt(k_own, qs[part]) * SCALE
            head = 2 * p + h
            pt = jnp.where(mask_t, jnp.exp(st), 0.0) * (1.0 / stats[head : head + 1])
            dst = pt * (dot_nt(v_own, gs[part]) - stats[HEADS + head : HEADS + head + 1])
            dk = dk + dot(dst.astype(BF16), qs[part])
            dv = dv + dot(pt.astype(BF16), gs[part])
        dk_p.append(dk * SCALE)
        dv_p.append(dv)
    join = lambda parts: jnp.concatenate(parts, axis=1)
    dq = head_back(join(dq_p), unit_q[...], scale_q[...]).astype(BF16)
    dk = head_back(join(dk_p), unit_k[...], scale_k[...]).astype(BF16)
    dv = join(dv_p).astype(BF16)
    total = dot_nt(dq, w_ref[0]) + dot_nt(dk, w_ref[1]) + dot_nt(dv, w_ref[2])
    normed, factor = rms_rows(x_ref[...].astype(F32))
    grad_ref[...] = (hg_ref[...] + row_back(total, normed, factor)).astype(BF16)


def per_device(tokens, cotangent, fine_qkv, fine_out, coarse_qkv, coarse_out):
    rows = tokens.shape[0]
    hops = -(-WINDOW // rows)
    outs = rows // POOL
    me, count, subs = place()
    pos = jnp.stack([me, jnp.int32(count)]).astype(jnp.int32)
    far = (hops + 2) * outs
    shape = jax.ShapeDtypeStruct
    dma = pltpu.SemaphoreType.DMA
    fine_w = jnp.transpose(fine_qkv, (1, 0, 2))
    coarse_w = jnp.transpose(coarse_qkv, (1, 0, 2))
    coarse_grad = cotangent.astype(F32).reshape(outs, POOL, D).sum(axis=1).astype(BF16)
    before, after, cg_all = comm(
        functools.partial(first_exchange, hops),
        (shape((hops, rows, D), BF16), shape((hops, rows, D), BF16), shape((count, outs, D), BF16)),
        [dma((2 * hops,)), dma((2 * hops,)), dma((count,)), dma((count,)), dma],
        0, [VMEM, VMEM], tokens, coarse_grad,
    )
    length = (hops + 1) * rows
    flat = lambda a: a.reshape(-1, D)
    q_all, k_all, v_all, unit_q, unit_k, scale_q, scale_k, totals, attended, hidden = local_call(
        fine_forward,
        [shape((length, D), BF16)] * 3 + [shape((rows, D), F32)] * 4
        + [shape((rows, 128), F32)] + [shape((rows, D), BF16)] * 2,
        pos, flat(before), tokens, flat(after), fine_w, fine_out,
    )
    pooled_all, cot_after = comm(
        functools.partial(second_exchange, hops),
        (shape((count, outs, D), BF16), shape((hops, rows, D), BF16)),
        [pltpu.VMEM((POOL, D), BF16), pltpu.VMEM((outs, D), BF16), dma((hops + 1,)), dma((hops + 1,)),
         dma((count,)), dma((count,)), dma],
        1, [VMEM, VMEM], hidden, cotangent,
    )
    pooled_all, cg_all = flat(pooled_all), flat(cg_all)
    mixed_all, grad_all = local_call(
        coarse_level,
        [shape((count * outs, D), BF16), shape((count * outs + far, D), BF16)],
        pos, pooled_all, cg_all, coarse_w, coarse_out,
    )
    mixed_in, grad_in = comm(
        functools.partial(third_exchange, far),
        (shape((subs, outs, D), BF16), shape((subs, far, D), BF16)),
        [dma((2 * subs,)), dma((2 * subs,)), dma((2,))],
        2, [VMEM, VMEM], mixed_all, grad_all,
    )
    tail = lambda a: lax.dynamic_slice_in_dim(jnp.pad(a, ((0, far), (0, 0))), me * outs, far)
    output, hidden_grad, g_all, delta, stats = local_call(
        middle,
        [shape((rows, D), BF16), shape((rows, D), F32), shape((length, D), BF16),
         shape((rows, 128), F32), shape((2 * HEADS, rows), F32)],
        pos, hidden, mixed_in, grad_in, tail(pooled_all), tail(cg_all), cotangent, flat(cot_after),
        attended, totals, fine_out,
    )
    stats_after = comm(
        functools.partial(fourth_exchange, hops),
        shape((hops, 2 * HEADS, rows), F32),
        [dma((hops,)), dma((hops,))],
        3, [VMEM], stats,
    )
    grad_tokens = local_call(
        fine_backward, shape((rows, D), BF16),
        pos, tokens, fine_w, q_all, k_all, v_all, g_all, stats, stats_after, totals, delta,
        unit_q, unit_k, scale_q, scale_k, hidden_grad,
    )
    return (output, grad_tokens)


def solution(mesh):
    placed = (
        P(("seq", "sub"), None),
        P(("seq", "sub"), None),
        P(),
        P(),
        P(None, None, "sub"),
        P("sub", None),
    )
    return jax.shard_map(
        per_device,
        mesh=mesh,
        in_specs=placed,
        out_specs=(P(("seq", "sub"), None), P(("seq", "sub"), None)),
        check_vma=False,
    )
```

```python
import functools

import jax
import jax.numpy as jnp
from jax import lax
from jax.experimental import pallas as pl
from jax.experimental.pallas import tpu as pltpu
from jax.sharding import PartitionSpec as P

D = 1024
HEADS = 16
HEAD_DIM = 64
WINDOW = 512
POOL = 16
EPS = 1e-06
F32 = jnp.float32
BF16 = jnp.bfloat16
MESH = pl.DeviceIdType.MESH
PAIR = 2 * HEAD_DIM
SCALE = HEAD_DIM ** (-0.5)
VMEM = pl.BlockSpec(memory_space=pltpu.VMEM)
ANY = pl.BlockSpec(memory_space=pl.ANY)
SMEM = pl.BlockSpec(memory_space=pltpu.SMEM)


def dot(a, b):
    return jnp.dot(a, b, preferred_element_type=F32)


def dot_nt(a, b):
    return lax.dot_general(a, b, (((1,), (1,)), ((), ())), preferred_element_type=F32)


def dot_tn(a, b):
    return lax.dot_general(a, b, (((0,), (0,)), ((), ())), preferred_element_type=F32)


def split(x):
    hi = x.astype(BF16)
    return hi, (x - hi.astype(F32)).astype(BF16)


def iota(shape, axis):
    return lax.broadcasted_iota(jnp.int32, shape, axis)


def head_sum(x):
    group = (iota((x.shape[1], 128), 0) // HEAD_DIM == iota((x.shape[1], 128), 1)).astype(F32).astype(BF16)
    hi, lo = split(x)
    return dot(hi, group) + dot(lo, group)


def head_spread(f, width):
    group = (iota((128, width), 1) // HEAD_DIM == iota((128, width), 0)).astype(F32).astype(BF16)
    hi, lo = split(f)
    return dot(hi, group) + dot(lo, group)


def head_rms(raw):
    factor = lax.rsqrt(head_sum(raw * raw) / HEAD_DIM + EPS)
    factor = head_spread(factor, raw.shape[1])
    return raw * factor, factor


def head_back(grad, unit, factor):
    return factor * (grad - unit * head_spread(head_sum(unit * grad) / HEAD_DIM, grad.shape[1]))


def rms_rows(x):
    factor = lax.rsqrt(jnp.mean(x * x, axis=-1, keepdims=True) + EPS)
    return x * factor, factor


def row_back(grad, normed, factor):
    return factor * (grad - normed * jnp.mean(normed * grad, axis=-1, keepdims=True))


def both(pair):
    low = iota(pair.shape, 1) < HEAD_DIM
    wide = pair.astype(F32)
    return jnp.concatenate([jnp.where(low, wide, 0.0), jnp.where(low, 0.0, wide)]).astype(BF16)


def pick(stacked):
    half = stacked.shape[0] // 2
    low = iota((half, PAIR), 1) < HEAD_DIM
    return jnp.where(low, stacked[:half], stacked[half:])


def place():
    subs = lax.axis_size("sub")
    count = lax.axis_size("seq") * subs
    me = lax.axis_index("seq") * subs + lax.axis_index("sub")
    return me, count, subs


def coords(index, subs):
    return (index // subs, index % subs)


def greet_all():
    me, count, subs = place()
    barrier = pltpu.get_barrier_semaphore()

    @pl.loop(1, count)
    def _(k):
        pl.semaphore_signal(
            barrier, inc=1, device_id=coords((me + k) % count, subs), device_id_type=MESH
        )

    pl.semaphore_wait(barrier, count - 1)


def remote(src, dst, send, recv, target, subs):
    return pltpu.make_async_remote_copy(
        src_ref=src, dst_ref=dst, send_sem=send, recv_sem=recv,
        device_id=coords(target, subs), device_id_type=MESH,
    )


class Spread:
    def __init__(self, src, dst, out_sem, mid_sem, last_sem, sent):
        self.me, self.count, self.subs = place()
        self.cores = 2 if lax.axis_size("seq") % 2 == 0 else 1
        self.groups = self.count // self.subs // self.cores
        self.sub = self.me % self.subs
        self.core = self.me // self.subs % self.cores
        self.group = self.me // self.subs // self.cores
        self.src, self.dst, self.sems, self.sent = src, dst, (out_sem, mid_sem, last_sem), sent

    def index(self, k, core, j):
        group = (self.group + self.groups - k) % self.groups
        sub = (self.sub + self.subs - j) % self.subs
        return (group * self.cores + (self.core + core) % self.cores) * self.subs + sub

    def copy(self, phase, j, k):
        if phase == 0:
            spot, source = self.me, self.src
            target, sem = self.index(self.groups - k, 0, 0), self.sems[0].at[k]
        elif phase == 1:
            spot = self.index(k, 0, 0)
            target, sem = self.index(0, 0, self.subs - j), self.sems[1].at[j, k]
        else:
            spot = self.index(k, 0, j)
            target, sem = self.index(0, 1, 0), self.sems[2].at[j, k]
        source = self.src if phase == 0 else self.dst.at[spot]
        return remote(source, self.dst.at[spot], self.sent.at[phase, j, k], sem, target, self.subs)

    def arrive(self, phase, j, k):
        if phase == 0:
            spot, sem = self.index(k, 0, 0), self.sems[0].at[k]
        elif phase == 1:
            spot, sem = self.index(k, 0, j), self.sems[1].at[j, k]
        else:
            spot, sem = self.index(k, 1, j), self.sems[2].at[j, k]
        other = (self.me + 1) % self.count
        return remote(self.dst.at[spot], self.dst.at[spot], self.sent.at[phase, j, k], sem, other, self.subs)

    def relay(self, k):
        for j in range(1, self.subs):
            self.copy(1, j, k).start()
        if self.cores > 1:
            self.copy(2, 0, k).start()

    def start(self):
        self.dst[self.me] = self.src[...]

        @pl.loop(1, self.groups)
        def _(k):
            self.copy(0, 0, k).start()

        self.relay(0)

    def finish(self):
        @pl.loop(1, self.groups)
        def _(k):
            self.arrive(0, 0, k).wait_recv()
            self.relay(k)

        @pl.loop(0, self.groups)
        def _(k):
            for j in range(1, self.subs):
                self.arrive(1, j, k).wait_recv()
                if self.cores > 1:
                    self.copy(2, j, k).start()

        @pl.loop(0, self.groups)
        def _(k):
            for j in range(self.subs):
                if self.cores > 1:
                    self.arrive(2, j, k).wait_recv()
                    self.copy(2, j, k).wait_send()
                if j > 0:
                    self.copy(1, j, k).wait_send()

        @pl.loop(1, self.groups)
        def _(k):
            self.copy(0, 0, k).wait_send()


def spread_sems(count, subs):
    cores = 2 if count // subs % 2 == 0 else 1
    groups = count // subs // cores
    dma = pltpu.SemaphoreType.DMA
    return [dma((groups,)), dma((subs, groups)), dma((subs, groups)), dma((3, subs, groups))]


class Halo:
    def __init__(self, src, dst, sends, recvs, hops, sign):
        self.me, self.count, self.subs = place()
        self.src, self.dst, self.sends, self.recvs = src, dst, sends, recvs
        self.hops, self.sign = hops, sign
        self.paired = lax.axis_size("seq") % 2 == 0
        far_core = self.me // self.subs % 2
        self.first = far_core == (0 if sign > 0 else 1)

    def slot(self, d):
        return self.dst.at[self.hops - d if self.sign > 0 else d - 1]

    def inside(self, index):
        return (index >= 0) & (index < self.count)

    def cuts(self, d):
        if not self.paired or d <= self.subs:
            return self.inside(self.me + self.sign * d)
        target = self.me + self.sign * d + 2 * self.count * self.subs
        core = target // self.subs % 2
        return self.inside(self.me + self.sign * d) & (core == (0 if self.sign > 0 else 1))

    def direct(self, d):
        target = jnp.clip(self.me + self.sign * d, 0, self.count - 1)
        return remote(self.src, self.slot(d), self.sends.at[d - 1], self.recvs.at[d - 1], target, self.subs)

    def passed(self, d):
        target = jnp.clip(self.me + self.sign * self.subs, 0, self.count - 1)
        to = d + self.subs
        return remote(
            self.slot(d), self.slot(to), self.sends.at[self.hops + to - 1], self.recvs.at[to - 1],
            target, self.subs,
        )

    def relays(self, d):
        return self.first & self.inside(self.me - self.sign * d)

    def start(self):
        for d in range(1, self.hops + 1):
            @pl.when(self.cuts(d))
            def _():
                self.direct(d).start()

    def finish(self):
        for d in range(1, self.hops + 1):
            @pl.when(self.inside(self.me - self.sign * d))
            def _():
                self.direct(d).wait_recv()

            if self.paired and d + self.subs <= self.hops:
                @pl.when(self.relays(d))
                def _():
                    self.passed(d).start()

    def drain(self):
        for d in range(1, self.hops + 1):
            @pl.when(self.cuts(d))
            def _():
                self.direct(d).wait_send()

            if self.paired and d + self.subs <= self.hops:
                @pl.when(self.relays(d))
                def _():
                    self.passed(d).wait_send()


class Shift:
    def __init__(self, src, dst, send, recv, distance):
        me, count, subs = place()
        self.me, self.subs, self.target = me, subs, me + distance
        self.args = (src, dst, send, recv)
        self.sends = (me + distance >= 0) & (me + distance < count)
        self.gets = (me - distance >= 0) & (me - distance < count)
        self.copy = remote(src, dst, send, recv, jnp.clip(me + distance, 0, count - 1), subs)

    def start(self):
        @pl.when(self.sends)
        def _():
            self.copy.start()

    def wait(self):
        @pl.when(self.sends)
        def _():
            self.copy.wait_send()

        @pl.when(self.gets)
        def _():
            self.copy.wait_recv()


def comm(body, outs, scratch, ident, specs, *args, out_specs=None):
    return pl.pallas_call(
        body,
        out_shape=outs,
        in_specs=specs,
        out_specs=jax.tree.map(lambda _: ANY, outs) if out_specs is None else out_specs,
        scratch_shapes=scratch,
        compiler_params=pltpu.CompilerParams(
            collective_id=ident, has_side_effects=True, vmem_limit_bytes=60 * 1024 * 1024
        ),
    )(*args)


def local_call(body, outs, *args, smem=True):
    return pl.pallas_call(
        body,
        out_shape=outs,
        in_specs=[SMEM] + [VMEM] * (len(args) - 1),
        out_specs=jax.tree.map(lambda _: VMEM, outs),
        compiler_params=pltpu.CompilerParams(vmem_limit_bytes=60 * 1024 * 1024),
    )(*args)


def second_exchange(hidden_ref, pooled_all, tail, pooled, send, recv, *sems):
    me, count, subs = place()
    rows = hidden_ref.shape[0]
    outs = rows // POOL
    greet_all()
    carry = Shift(hidden_ref.at[pl.ds(rows - POOL, POOL)], tail, send, recv, 1)
    carry.start()
    back = iota((outs, rows), 0) * POOL - iota((outs, rows), 1)
    part = dot(((back >= 0) & (back < POOL)).astype(F32).astype(BF16), hidden_ref[...])
    carry.wait()
    lead = (iota((outs, POOL), 0) == 0) & (iota((outs, POOL), 1) > 0)
    tail_rows = jnp.where(me > 0, tail[...].astype(F32), 0.0).astype(BF16)
    part = part + dot(lead.astype(F32).astype(BF16), tail_rows)
    pooled[...] = (part / POOL).astype(BF16)
    spread = Spread(pooled, pooled_all, *sems)
    spread.start()
    spread.finish()


def third_exchange(far, mixed_all, grad_all, mixed_in, grad_in, sends, recvs, local):
    me, count, subs = place()
    mine = lax.axis_index("sub")
    seq = lax.axis_index("seq")
    outs = mixed_in.shape[1]
    barrier = pltpu.get_barrier_semaphore()
    for k in range(1, subs):
        pl.semaphore_signal(
            barrier, inc=1, device_id=(seq, (mine + k) % subs), device_id_type=MESH
        )
    pl.semaphore_wait(barrier, subs - 1)
    copies = []
    for k in range(1, subs):
        target = seq * subs + (mine + k) % subs
        start = pl.multiple_of(target * outs, outs)
        pieces = (
            (mixed_all.at[pl.ds(start, outs)], mixed_in.at[k]),
            (grad_all.at[pl.ds(start, far)], grad_in.at[k]),
        )
        for which, (src, dst) in enumerate(pieces):
            copies.append(remote(src, dst, sends.at[2 * k + which], recvs.at[2 * k + which], target, subs))
    for copy in copies:
        copy.start()
    start = pl.multiple_of(me * outs, outs)
    own = [
        pltpu.make_async_copy(mixed_all.at[pl.ds(start, outs)], mixed_in.at[0], local.at[0]),
        pltpu.make_async_copy(grad_all.at[pl.ds(start, far)], grad_in.at[0], local.at[1]),
    ]
    for copy in own:
        copy.start()
    for copy in copies + own:
        copy.wait()


def fourth_exchange(hops, stats_ref, after, sends, recvs):
    me, count, subs = place()
    barrier = pltpu.get_barrier_semaphore()
    for d in range(1, hops + 1):
        for other in (me - d, me + d):

            @pl.when((other >= 0) & (other < count))
            def _():
                pl.semaphore_signal(
                    barrier, inc=1, device_id=coords(jnp.clip(other, 0, count - 1), subs),
                    device_id_type=MESH,
                )

    pl.semaphore_wait(barrier, jnp.minimum(me, hops) + jnp.minimum(count - 1 - me, hops))

    moves = [
        Shift(stats_ref, after.at[d - 1], sends.at[d - 1], recvs.at[d - 1], -d)
        for d in range(1, hops + 1)
    ]
    for move in moves:
        move.start()
    for move in moves:
        move.wait()


def window_mask(rows, keys, anchor):
    gap = keys - rows + iota((rows, keys), 0) - iota((rows, keys), 1)
    return (gap >= 0) & (gap < WINDOW) & (anchor - (keys - rows) + iota((rows, keys), 1) >= 0)


def fine_forward(
    hops, x_ref, cot_ref, cg_ref, w_hbm, out_hbm,
    q_all, k_all, v_all, unit_q, unit_k, scale_q, scale_k, tot_ref, att_ref, hidden_ref, cg_all,
    after, cot_after,
    before, w_ref, out_w, load, sends, recvs, *sems,
):
    me, count, subs = place()
    rows = x_ref.shape[0]
    margin = hops * rows
    anchor = me * rows
    loads = [
        pltpu.make_async_copy(w_hbm, w_ref, load.at[0]),
        pltpu.make_async_copy(out_hbm, out_w, load.at[1]),
    ]
    for one in loads:
        one.start()
    greet_all()
    down = Halo(x_ref, before, sends.at[0], recvs.at[0], hops, 1)
    up = Halo(x_ref, after, sends.at[1], recvs.at[1], hops, -1)
    up_cot = Halo(cot_ref, cot_after, sends.at[2], recvs.at[2], hops, -1)
    spread = Spread(cg_ref, cg_all, *sems)
    down.start()
    up.start()
    up_cot.start()
    spread.start()
    own = x_ref[...].astype(F32)
    own_b = rms_rows(own)[0].astype(BF16)
    loads[0].wait()
    unit, factor = head_rms(dot(own_b, w_ref[0]))
    q_all[...] = unit.astype(BF16)
    unit_q[...] = unit
    scale_q[...] = factor
    unit, factor = head_rms(dot(own_b, w_ref[1]))
    k_all[pl.ds(margin, rows), :] = unit.astype(BF16)
    unit_k[...] = unit
    scale_k[...] = factor
    v_all[pl.ds(margin, rows), :] = dot(own_b, w_ref[2]).astype(BF16)
    down.finish()
    prev = before[...].reshape(margin, D).astype(F32)
    prev = jnp.where(anchor - margin + iota(prev.shape, 0) >= 0, prev, 0.0)
    prev_b = rms_rows(prev)[0].astype(BF16)
    k_all[pl.ds(0, margin), :] = head_rms(dot(prev_b, w_ref[1]))[0].astype(BF16)
    v_all[pl.ds(0, margin), :] = dot(prev_b, w_ref[2]).astype(BF16)
    mask = window_mask(rows, margin + rows, anchor)
    mask = jnp.concatenate([mask.astype(F32)] * 2) > 0
    lane = iota((rows, 128), 1)
    totals = jnp.ones((rows, 128), F32)
    for p in range(HEADS // 2):
        cols = pl.ds(p * PAIR, PAIR)
        s = dot_nt(both(q_all[pl.ds(0, rows), cols]), k_all[:, cols]) * SCALE
        e = jnp.where(mask, jnp.exp(s), 0.0)
        t = jnp.sum(e, axis=-1, keepdims=True)
        prob = (e * (1.0 / t)).astype(BF16)
        att_ref[:, cols] = pick(dot(prob, v_all[:, cols])).astype(BF16)
        totals = jnp.where(lane == 2 * p, t[:rows], totals)
        totals = jnp.where(lane == 2 * p + 1, t[rows:], totals)
    tot_ref[...] = totals
    loads[1].wait()
    hidden_ref[...] = (own + dot(att_ref[...], out_w[...])).astype(BF16)
    up.finish()
    up_cot.finish()
    spread.finish()
    down.drain()
    up.drain()
    up_cot.drain()


def coarse_level(pos, pooled_ref, cg_ref, w_ref, out_w, mixed_ref, grad_ref):
    count, width = pooled_ref.shape[0], w_ref.shape[2]
    normed_b = rms_rows(pooled_ref[...].astype(F32))[0].astype(BF16)
    uq, fq = head_rms(dot(normed_b, w_ref[0]))
    uk, fk = head_rms(dot(normed_b, w_ref[1]))
    qb, kb = uq.astype(BF16), uk.astype(BF16)
    vb = dot(normed_b, w_ref[2]).astype(BF16)
    gb = dot_nt(cg_ref[...], out_w[...]).astype(BF16)
    block = min(count, 256)
    att_p, dq_p, dk_p, dv_p = [], [], [], []
    for p in range(width // PAIR):
        cols = slice(p * PAIR, (p + 1) * PAIR)
        att_b, dq_b, dk, dv = [], [], None, None
        kp, vp = kb[:, cols], vb[:, cols]
        for b in range(count // block):
            rows = slice(b * block, (b + 1) * block)
            qs, gs = both(qb[rows, cols]), both(gb[rows, cols])
            s = dot_nt(qs, kp) * SCALE
            where = iota((2 * block, count), 0) % block + b * block >= iota((2 * block, count), 1)
            e = jnp.where(where, jnp.exp(s), 0.0)
            full = e * (1.0 / jnp.sum(e, axis=-1, keepdims=True))
            prob = full.astype(BF16)
            att = pick(dot(prob, vp)).astype(BF16)
            att_b.append(att)
            att2 = jnp.concatenate([att.astype(F32)] * 2)
            delta = jnp.sum(gs.astype(F32) * att2, axis=-1, keepdims=True)
            ds = (full * (dot_nt(gs, vp) - delta)).astype(BF16)
            dq_b.append(pick(dot(ds, kp)) * SCALE)
            dk_t, dv_t = dot_tn(ds, qs) * SCALE, dot_tn(prob, gs)
            dk = dk_t if dk is None else dk + dk_t
            dv = dv_t if dv is None else dv + dv_t
        att_p.append(jnp.concatenate(att_b))
        dq_p.append(jnp.concatenate(dq_b))
        dk_p.append(dk)
        dv_p.append(dv)
    join = lambda parts: jnp.concatenate(parts, axis=1)
    mixed_ref[...] = dot(join(att_p), out_w[...]).astype(BF16)
    dq = head_back(join(dq_p), uq, fq).astype(BF16)
    dk = head_back(join(dk_p), uk, fk).astype(BF16)
    dv = join(dv_p).astype(BF16)
    total = dot_nt(dq, w_ref[0]) + dot_nt(dk, w_ref[1]) + dot_nt(dv, w_ref[2])
    grad_ref[pl.ds(0, count), :] = total.astype(BF16)
    extra = grad_ref.shape[0] - count
    grad_ref[pl.ds(count, extra), :] = jnp.zeros((extra, D), BF16)


def middle(
    pos, hidden_ref, mixed_in, grad_in, pooled_ref, cg_ref, cot_ref, cot_after, att_ref, tot_ref, out_w,
    output_ref, hg_ref, g_all, delta_ref, stats_ref,
):
    rows = hidden_ref.shape[0]
    outs = rows // POOL
    ahead = cot_after.shape[0]
    far = grad_in.shape[1]
    start = pos[0] * rows
    pooled = pooled_ref[...].astype(F32)
    mixed = jnp.sum(mixed_in[...].astype(F32), axis=0)
    state = (pooled[:outs] + mixed).astype(BF16)
    onto = (iota((rows, outs), 0) // POOL == iota((rows, outs), 1)).astype(F32).astype(BF16)
    output_ref[...] = (hidden_ref[...].astype(F32) + dot(onto, state)).astype(BF16)
    nxt = cot_after[...].astype(F32)
    nxt = jnp.where(start + rows + iota(nxt.shape, 0) < pos[1] * rows, nxt, 0.0)
    cot = jnp.concatenate([cot_ref[...].astype(F32), nxt])
    length = rows + ahead
    near = length // POOL
    groups = (iota((near, length), 1) // POOL == iota((near, length), 0)).astype(F32).astype(BF16)
    cg = jnp.concatenate([dot(groups, cot.astype(BF16)), cg_ref[...].astype(F32)[near:]])
    ng = jnp.sum(grad_in[...].astype(F32), axis=0)
    normed, factor = rms_rows(pooled)
    pg = (cg + row_back(ng, normed, factor)) / POOL
    pg = jnp.where(pos[0] * outs + iota(pg.shape, 0) < pos[1] * outs, pg, 0.0)
    lift = ((iota((length, far), 0) + POOL - 1) // POOL == iota((length, far), 1)).astype(F32).astype(BF16)
    hi, lo = split(pg)
    hidden_grad = cot + dot(lift, hi) + dot(lift, lo)
    hg_ref[...] = hidden_grad[:rows]
    g_all[...] = dot_nt(hidden_grad.astype(BF16), out_w[...]).astype(BF16)
    delta = head_sum(g_all[pl.ds(0, rows), :].astype(F32) * att_ref[...].astype(F32))
    delta_ref[...] = delta
    stats_ref[pl.ds(0, HEADS), :] = tot_ref[...].T[:HEADS]
    stats_ref[pl.ds(HEADS, HEADS), :] = delta.T[:HEADS]


def fine_backward(
    pos, x_ref, next_ref, w_ref, q_own, k_all, v_all, g_all, own_stats, after, tot_ref, delta_ref,
    unit_q, unit_k, scale_q, scale_k, hg_ref, grad_ref,
):
    rows = x_ref.shape[0]
    hops = after.shape[0]
    margin = k_all.shape[0] - rows
    length = g_all.shape[0]
    anchor = pos[0] * rows
    nxt = next_ref[...].astype(F32)
    nxt = jnp.where(anchor + rows + iota(nxt.shape, 0) < pos[1] * rows, nxt, 0.0)
    q_next = head_rms(dot(rms_rows(nxt)[0].astype(BF16), w_ref[0]))[0].astype(BF16)
    q_all = jnp.concatenate([q_own[...], q_next])
    mask = window_mask(rows, margin + rows, anchor)
    mask = jnp.concatenate([mask.astype(F32)] * 2) > 0
    gap = iota((rows, length), 1) - iota((rows, length), 0)
    mask_t = (gap >= 0) & (gap < WINDOW) & (anchor + iota((rows, length), 1) < pos[1] * rows)
    stats = jnp.concatenate([own_stats[...]] + [after[d] for d in range(hops)], axis=1)
    stats = jnp.where(anchor + iota(stats.shape, 1) < pos[1] * rows, stats, 1.0)
    totals, deltas = tot_ref[...], delta_ref[...]
    dq_p, dk_p, dv_p = [], [], []
    for p in range(HEADS // 2):
        cols = pl.ds(p * PAIR, PAIR)
        kp, vp, gp = k_all[:, cols], v_all[:, cols], g_all[:, cols]
        qp = q_all[:, p * PAIR : (p + 1) * PAIR]
        s = dot_nt(both(qp[:rows]), kp) * SCALE
        e = jnp.where(mask, jnp.exp(s), 0.0)
        column = lambda m: jnp.concatenate([m[:, 2 * p : 2 * p + 1], m[:, 2 * p + 1 : 2 * p + 2]])
        ds = e * (1.0 / column(totals)) * (dot_nt(both(gp[:rows]), vp) - column(deltas))
        dq_p.append(pick(dot(ds.astype(BF16), kp)) * SCALE)
        k_own, v_own = kp[margin:], vp[margin:]
        qs, gs = both(qp), both(gp)
        dk = dv = jnp.zeros((rows, PAIR), F32)
        for h in range(2):
            part = slice(h * length, (h + 1) * length)
            st = dot_nt(k_own, qs[part]) * SCALE
            head = 2 * p + h
            pt = jnp.where(mask_t, jnp.exp(st), 0.0) * (1.0 / stats[head : head + 1])
            dst = pt * (dot_nt(v_own, gs[part]) - stats[HEADS + head : HEADS + head + 1])
            dk = dk + dot(dst.astype(BF16), qs[part])
            dv = dv + dot(pt.astype(BF16), gs[part])
        dk_p.append(dk * SCALE)
        dv_p.append(dv)
    join = lambda parts: jnp.concatenate(parts, axis=1)
    dq = head_back(join(dq_p), unit_q[...], scale_q[...]).astype(BF16)
    dk = head_back(join(dk_p), unit_k[...], scale_k[...]).astype(BF16)
    dv = join(dv_p).astype(BF16)
    total = dot_nt(dq, w_ref[0]) + dot_nt(dk, w_ref[1]) + dot_nt(dv, w_ref[2])
    normed, factor = rms_rows(x_ref[...].astype(F32))
    grad_ref[...] = (hg_ref[...] + row_back(total, normed, factor)).astype(BF16)


def per_device(tokens, cotangent, fine_qkv, fine_out, coarse_qkv, coarse_out):
    rows = tokens.shape[0]
    hops = -(-WINDOW // rows)
    outs = rows // POOL
    me, count, subs = place()
    pos = jnp.stack([me, jnp.int32(count)]).astype(jnp.int32)
    far = (hops + 2) * outs
    shape = jax.ShapeDtypeStruct
    dma = pltpu.SemaphoreType.DMA
    fine_w = jnp.transpose(fine_qkv, (1, 0, 2))
    coarse_w = jnp.transpose(coarse_qkv, (1, 0, 2))
    coarse_grad = cotangent.astype(F32).reshape(outs, POOL, D).sum(axis=1).astype(BF16)
    length = (hops + 1) * rows
    flat = lambda a: a.reshape(-1, D)
    q_own, k_all, v_all, unit_q, unit_k, scale_q, scale_k, totals, attended, hidden, cg_all, after, cot_after = comm(
        functools.partial(fine_forward, hops),
        [shape((rows, D), BF16)] + [shape((length, D), BF16)] * 2 + [shape((rows, D), F32)] * 4
        + [shape((rows, 128), F32)] + [shape((rows, D), BF16)] * 2
        + [shape((count, outs, D), BF16)] + [shape((hops, rows, D), BF16)] * 2,
        [pltpu.VMEM((hops, rows, D), BF16), pltpu.VMEM(fine_w.shape, BF16), pltpu.VMEM(fine_out.shape, BF16),
         dma((2,)), dma((3, 2 * hops)), dma((3, hops))] + spread_sems(count, subs),
        0, [VMEM] * 3 + [ANY] * 2, tokens, cotangent, coarse_grad, fine_w, fine_out,
        out_specs=[VMEM] * 13,
    )
    pooled_all = comm(
        second_exchange,
        shape((count, outs, D), BF16),
        [pltpu.VMEM((POOL, D), BF16), pltpu.VMEM((outs, D), BF16), dma, dma] + spread_sems(count, subs),
        1, [VMEM], hidden, out_specs=VMEM,
    )
    pooled_all, cg_all = flat(pooled_all), flat(cg_all)
    mixed_all, grad_all = local_call(
        coarse_level,
        [shape((count * outs, D), BF16), shape((count * outs + far, D), BF16)],
        pos, pooled_all, cg_all, coarse_w, coarse_out,
    )
    mixed_in, grad_in = comm(
        functools.partial(third_exchange, far),
        (shape((subs, outs, D), BF16), shape((subs, far, D), BF16)),
        [dma((2 * subs,)), dma((2 * subs,)), dma((2,))],
        2, [VMEM, VMEM], mixed_all, grad_all,
    )
    tail = lambda a: lax.dynamic_slice_in_dim(jnp.pad(a, ((0, far), (0, 0))), me * outs, far)
    output, hidden_grad, g_all, delta, stats = local_call(
        middle,
        [shape((rows, D), BF16), shape((rows, D), F32), shape((length, D), BF16),
         shape((rows, 128), F32), shape((2 * HEADS, rows), F32)],
        pos, hidden, mixed_in, grad_in, tail(pooled_all), tail(cg_all), cotangent, flat(cot_after),
        attended, totals, fine_out,
    )
    stats_after = comm(
        functools.partial(fourth_exchange, hops),
        shape((hops, 2 * HEADS, rows), F32),
        [dma((hops,)), dma((hops,))],
        3, [VMEM], stats,
    )
    grad_tokens = local_call(
        fine_backward, shape((rows, D), BF16),
        pos, tokens, flat(after), fine_w, q_own, k_all, v_all, g_all, stats, stats_after, totals, delta,
        unit_q, unit_k, scale_q, scale_k, hidden_grad,
    )
    return (output, grad_tokens)


def solution(mesh):
    placed = (
        P(("seq", "sub"), None),
        P(("seq", "sub"), None),
        P(),
        P(),
        P(None, None, "sub"),
        P("sub", None),
    )
    return jax.shard_map(
        per_device,
        mesh=mesh,
        in_specs=placed,
        out_specs=(P(("seq", "sub"), None), P(("seq", "sub"), None)),
        check_vma=False,
    )
```

```python
import functools

import jax
import jax.numpy as jnp
from jax import lax
from jax.experimental import pallas as pl
from jax.experimental.pallas import tpu as pltpu
from jax.sharding import PartitionSpec as P

D = 1024
HEADS = 16
HEAD_DIM = 64
WINDOW = 512
POOL = 16
EPS = 1e-06
F32 = jnp.float32
BF16 = jnp.bfloat16
MESH = pl.DeviceIdType.MESH
PAIR = 2 * HEAD_DIM
SCALE = HEAD_DIM ** (-0.5)
VMEM = pl.BlockSpec(memory_space=pltpu.VMEM)
ANY = pl.BlockSpec(memory_space=pl.ANY)
SMEM = pl.BlockSpec(memory_space=pltpu.SMEM)


def dot(a, b):
    return jnp.dot(a, b, preferred_element_type=F32)


def dot_nt(a, b):
    return lax.dot_general(a, b, (((1,), (1,)), ((), ())), preferred_element_type=F32)


def dot_tn(a, b):
    return lax.dot_general(a, b, (((0,), (0,)), ((), ())), preferred_element_type=F32)


def split(x):
    hi = x.astype(BF16)
    return hi, (x - hi.astype(F32)).astype(BF16)


def iota(shape, axis):
    return lax.broadcasted_iota(jnp.int32, shape, axis)


def head_sum(x):
    group = (iota((x.shape[1], 128), 0) // HEAD_DIM == iota((x.shape[1], 128), 1)).astype(F32).astype(BF16)
    hi, lo = split(x)
    return dot(hi, group) + dot(lo, group)


def head_spread(f, width):
    group = (iota((128, width), 1) // HEAD_DIM == iota((128, width), 0)).astype(F32).astype(BF16)
    hi, lo = split(f)
    return dot(hi, group) + dot(lo, group)


def head_rms(raw):
    factor = lax.rsqrt(head_sum(raw * raw) / HEAD_DIM + EPS)
    factor = head_spread(factor, raw.shape[1])
    return raw * factor, factor


def head_back(grad, unit, factor):
    return factor * (grad - unit * head_spread(head_sum(unit * grad) / HEAD_DIM, grad.shape[1]))


def rms_rows(x):
    factor = lax.rsqrt(jnp.mean(x * x, axis=-1, keepdims=True) + EPS)
    return x * factor, factor


def row_back(grad, normed, factor):
    return factor * (grad - normed * jnp.mean(normed * grad, axis=-1, keepdims=True))


def both(pair):
    low = iota(pair.shape, 1) < HEAD_DIM
    wide = pair.astype(F32)
    return jnp.concatenate([jnp.where(low, wide, 0.0), jnp.where(low, 0.0, wide)]).astype(BF16)


def pick(stacked):
    half = stacked.shape[0] // 2
    low = iota((half, PAIR), 1) < HEAD_DIM
    return jnp.where(low, stacked[:half], stacked[half:])


def place():
    subs = lax.axis_size("sub")
    count = lax.axis_size("seq") * subs
    me = lax.axis_index("seq") * subs + lax.axis_index("sub")
    return me, count, subs


def coords(index, subs):
    return (index // subs, index % subs)


def greet_all():
    me, count, subs = place()
    barrier = pltpu.get_barrier_semaphore()

    @pl.loop(1, count)
    def _(k):
        pl.semaphore_signal(
            barrier, inc=1, device_id=coords((me + k) % count, subs), device_id_type=MESH
        )

    pl.semaphore_wait(barrier, count - 1)


def remote(src, dst, send, recv, target, subs):
    return pltpu.make_async_remote_copy(
        src_ref=src, dst_ref=dst, send_sem=send, recv_sem=recv,
        device_id=coords(target, subs), device_id_type=MESH,
    )


class Spread:
    def __init__(self, src, dst, out_sem, mid_sem, last_sem, sent):
        self.me, self.count, self.subs = place()
        self.cores = 2 if lax.axis_size("seq") % 2 == 0 else 1
        self.groups = self.count // self.subs // self.cores
        self.sub = self.me % self.subs
        self.core = self.me // self.subs % self.cores
        self.group = self.me // self.subs // self.cores
        self.src, self.dst, self.sems, self.sent = src, dst, (out_sem, mid_sem, last_sem), sent

    def index(self, k, core, j):
        group = (self.group + self.groups - k) % self.groups
        sub = (self.sub + self.subs - j) % self.subs
        return (group * self.cores + (self.core + core) % self.cores) * self.subs + sub

    def copy(self, phase, j, k):
        if phase == 0:
            spot, source = self.me, self.src
            target, sem = self.index(self.groups - k, 0, 0), self.sems[0].at[k]
        elif phase == 1:
            spot = self.index(k, 0, 0)
            target, sem = self.index(0, 0, self.subs - j), self.sems[1].at[j, k]
        else:
            spot = self.index(k, 0, j)
            target, sem = self.index(0, 1, 0), self.sems[2].at[j, k]
        source = self.src if phase == 0 else self.dst.at[spot]
        return remote(source, self.dst.at[spot], self.sent.at[phase, j, k], sem, target, self.subs)

    def arrive(self, phase, j, k):
        if phase == 0:
            spot, sem = self.index(k, 0, 0), self.sems[0].at[k]
        elif phase == 1:
            spot, sem = self.index(k, 0, j), self.sems[1].at[j, k]
        else:
            spot, sem = self.index(k, 1, j), self.sems[2].at[j, k]
        other = (self.me + 1) % self.count
        return remote(self.dst.at[spot], self.dst.at[spot], self.sent.at[phase, j, k], sem, other, self.subs)

    def relay(self, k):
        for j in range(1, self.subs):
            self.copy(1, j, k).start()
        if self.cores > 1:
            self.copy(2, 0, k).start()

    def start(self):
        self.dst[self.me] = self.src[...]

        @pl.loop(1, self.groups)
        def _(k):
            self.copy(0, 0, k).start()

        self.relay(0)

    def finish(self):
        @pl.loop(1, self.groups)
        def _(k):
            self.arrive(0, 0, k).wait_recv()
            self.relay(k)

        @pl.loop(0, self.groups)
        def _(k):
            for j in range(1, self.subs):
                self.arrive(1, j, k).wait_recv()
                if self.cores > 1:
                    self.copy(2, j, k).start()

        @pl.loop(0, self.groups)
        def _(k):
            for j in range(self.subs):
                if self.cores > 1:
                    self.arrive(2, j, k).wait_recv()
                    self.copy(2, j, k).wait_send()
                if j > 0:
                    self.copy(1, j, k).wait_send()

        @pl.loop(1, self.groups)
        def _(k):
            self.copy(0, 0, k).wait_send()


def spread_sems(count, subs):
    cores = 2 if count // subs % 2 == 0 else 1
    groups = count // subs // cores
    dma = pltpu.SemaphoreType.DMA
    return [dma((groups,)), dma((subs, groups)), dma((subs, groups)), dma((3, subs, groups))]


class Halo:
    def __init__(self, src, dst, sends, recvs, hops, sign):
        self.me, self.count, self.subs = place()
        self.src, self.dst, self.sends, self.recvs = src, dst, sends, recvs
        self.hops, self.sign = hops, sign
        self.paired = lax.axis_size("seq") % 2 == 0
        far_core = self.me // self.subs % 2
        self.first = far_core == (0 if sign > 0 else 1)

    def slot(self, d):
        return self.dst.at[self.hops - d if self.sign > 0 else d - 1]

    def inside(self, index):
        return (index >= 0) & (index < self.count)

    def cuts(self, d):
        if not self.paired or d <= self.subs:
            return self.inside(self.me + self.sign * d)
        target = self.me + self.sign * d + 2 * self.count * self.subs
        core = target // self.subs % 2
        return self.inside(self.me + self.sign * d) & (core == (0 if self.sign > 0 else 1))

    def direct(self, d):
        target = jnp.clip(self.me + self.sign * d, 0, self.count - 1)
        return remote(self.src, self.slot(d), self.sends.at[d - 1], self.recvs.at[d - 1], target, self.subs)

    def passed(self, d):
        target = jnp.clip(self.me + self.sign * self.subs, 0, self.count - 1)
        to = d + self.subs
        return remote(
            self.slot(d), self.slot(to), self.sends.at[self.hops + to - 1], self.recvs.at[to - 1],
            target, self.subs,
        )

    def relays(self, d):
        return self.first & self.inside(self.me - self.sign * d)

    def start(self):
        for d in range(1, self.hops + 1):
            @pl.when(self.cuts(d))
            def _():
                self.direct(d).start()

    def finish(self):
        for d in range(1, self.hops + 1):
            @pl.when(self.inside(self.me - self.sign * d))
            def _():
                self.direct(d).wait_recv()

            if self.paired and d + self.subs <= self.hops:
                @pl.when(self.relays(d))
                def _():
                    self.passed(d).start()

    def drain(self):
        for d in range(1, self.hops + 1):
            @pl.when(self.cuts(d))
            def _():
                self.direct(d).wait_send()

            if self.paired and d + self.subs <= self.hops:
                @pl.when(self.relays(d))
                def _():
                    self.passed(d).wait_send()


class Shift:
    def __init__(self, src, dst, send, recv, distance):
        me, count, subs = place()
        self.me, self.subs, self.target = me, subs, me + distance
        self.args = (src, dst, send, recv)
        self.sends = (me + distance >= 0) & (me + distance < count)
        self.gets = (me - distance >= 0) & (me - distance < count)
        self.copy = remote(src, dst, send, recv, jnp.clip(me + distance, 0, count - 1), subs)

    def start(self):
        @pl.when(self.sends)
        def _():
            self.copy.start()

    def wait(self):
        @pl.when(self.sends)
        def _():
            self.copy.wait_send()

        @pl.when(self.gets)
        def _():
            self.copy.wait_recv()


def comm(body, outs, scratch, ident, specs, *args, out_specs=None):
    return pl.pallas_call(
        body,
        out_shape=outs,
        in_specs=specs,
        out_specs=jax.tree.map(lambda _: ANY, outs) if out_specs is None else out_specs,
        scratch_shapes=scratch,
        compiler_params=pltpu.CompilerParams(
            collective_id=ident, has_side_effects=True, vmem_limit_bytes=60 * 1024 * 1024
        ),
    )(*args)


def local_call(body, outs, *args, smem=True):
    return pl.pallas_call(
        body,
        out_shape=outs,
        in_specs=[SMEM] + [VMEM] * (len(args) - 1),
        out_specs=jax.tree.map(lambda _: VMEM, outs),
        compiler_params=pltpu.CompilerParams(vmem_limit_bytes=60 * 1024 * 1024),
    )(*args)


def second_exchange(hidden_ref, pooled_all, tail, pooled, send, recv, *sems):
    me, count, subs = place()
    rows = hidden_ref.shape[0]
    outs = rows // POOL
    greet_all()
    carry = Shift(hidden_ref.at[pl.ds(rows - POOL, POOL)], tail, send, recv, 1)
    carry.start()
    back = iota((outs, rows), 0) * POOL - iota((outs, rows), 1)
    part = dot(((back >= 0) & (back < POOL)).astype(F32).astype(BF16), hidden_ref[...])
    carry.wait()
    lead = (iota((outs, POOL), 0) == 0) & (iota((outs, POOL), 1) > 0)
    tail_rows = jnp.where(me > 0, tail[...].astype(F32), 0.0).astype(BF16)
    part = part + dot(lead.astype(F32).astype(BF16), tail_rows)
    pooled[...] = (part / POOL).astype(BF16)
    spread = Spread(pooled, pooled_all, *sems)
    spread.start()
    spread.finish()


def third_exchange(far, mixed_all, grad_all, mixed_in, grad_in, sends, recvs, local):
    me, count, subs = place()
    mine = lax.axis_index("sub")
    seq = lax.axis_index("seq")
    outs = mixed_in.shape[1]
    barrier = pltpu.get_barrier_semaphore()
    for k in range(1, subs):
        pl.semaphore_signal(
            barrier, inc=1, device_id=(seq, (mine + k) % subs), device_id_type=MESH
        )
    pl.semaphore_wait(barrier, subs - 1)
    copies = []
    for k in range(1, subs):
        target = seq * subs + (mine + k) % subs
        start = pl.multiple_of(target * outs, outs)
        pieces = (
            (mixed_all.at[pl.ds(start, outs)], mixed_in.at[k]),
            (grad_all.at[pl.ds(start, far)], grad_in.at[k]),
        )
        for which, (src, dst) in enumerate(pieces):
            copies.append(remote(src, dst, sends.at[2 * k + which], recvs.at[2 * k + which], target, subs))
    for copy in copies:
        copy.start()
    start = pl.multiple_of(me * outs, outs)
    own = [
        pltpu.make_async_copy(mixed_all.at[pl.ds(start, outs)], mixed_in.at[0], local.at[0]),
        pltpu.make_async_copy(grad_all.at[pl.ds(start, far)], grad_in.at[0], local.at[1]),
    ]
    for copy in own:
        copy.start()
    for copy in copies + own:
        copy.wait()


def fourth_exchange(hops, stats_ref, after, sends, recvs):
    me, count, subs = place()
    barrier = pltpu.get_barrier_semaphore()
    for d in range(1, hops + 1):
        for other in (me - d, me + d):

            @pl.when((other >= 0) & (other < count))
            def _():
                pl.semaphore_signal(
                    barrier, inc=1, device_id=coords(jnp.clip(other, 0, count - 1), subs),
                    device_id_type=MESH,
                )

    pl.semaphore_wait(barrier, jnp.minimum(me, hops) + jnp.minimum(count - 1 - me, hops))

    moves = [
        Shift(stats_ref, after.at[d - 1], sends.at[d - 1], recvs.at[d - 1], -d)
        for d in range(1, hops + 1)
    ]
    for move in moves:
        move.start()
    for move in moves:
        move.wait()


def window_mask(rows, keys, anchor):
    gap = keys - rows + iota((rows, keys), 0) - iota((rows, keys), 1)
    return (gap >= 0) & (gap < WINDOW) & (anchor - (keys - rows) + iota((rows, keys), 1) >= 0)


def fine_forward(
    hops, x_ref, cot_ref, cg_ref, w_hbm, out_hbm,
    q_all, k_all, v_all, unit_q, unit_k, scale_q, scale_k, tot_ref, att_ref, hidden_ref, cg_all,
    after, cot_after,
    before, w_ref, out_w, load, sends, recvs, *sems,
):
    me, count, subs = place()
    rows = x_ref.shape[0]
    margin = hops * rows
    anchor = me * rows
    loads = [
        pltpu.make_async_copy(w_hbm, w_ref, load.at[0]),
        pltpu.make_async_copy(out_hbm, out_w, load.at[1]),
    ]
    for one in loads:
        one.start()
    greet_all()
    down = Halo(x_ref, before, sends.at[0], recvs.at[0], hops, 1)
    up = Halo(x_ref, after, sends.at[1], recvs.at[1], hops, -1)
    up_cot = Halo(cot_ref, cot_after, sends.at[2], recvs.at[2], hops, -1)
    spread = Spread(cg_ref, cg_all, *sems)
    down.start()
    spread.start()
    own = x_ref[...].astype(F32)
    own_b = rms_rows(own)[0].astype(BF16)
    loads[0].wait()
    unit, factor = head_rms(dot(own_b, w_ref[0]))
    q_all[...] = unit.astype(BF16)
    unit_q[...] = unit
    scale_q[...] = factor
    unit, factor = head_rms(dot(own_b, w_ref[1]))
    k_all[pl.ds(margin, rows), :] = unit.astype(BF16)
    unit_k[...] = unit
    scale_k[...] = factor
    v_all[pl.ds(margin, rows), :] = dot(own_b, w_ref[2]).astype(BF16)
    down.finish()
    up.start()
    up_cot.start()
    prev = before[...].reshape(margin, D).astype(F32)
    prev = jnp.where(anchor - margin + iota(prev.shape, 0) >= 0, prev, 0.0)
    prev_b = rms_rows(prev)[0].astype(BF16)
    k_all[pl.ds(0, margin), :] = head_rms(dot(prev_b, w_ref[1]))[0].astype(BF16)
    v_all[pl.ds(0, margin), :] = dot(prev_b, w_ref[2]).astype(BF16)
    mask = window_mask(rows, margin + rows, anchor)
    mask = jnp.concatenate([mask.astype(F32)] * 2) > 0
    lane = iota((rows, 128), 1)
    totals = jnp.ones((rows, 128), F32)
    for p in range(HEADS // 2):
        cols = pl.ds(p * PAIR, PAIR)
        s = dot_nt(both(q_all[pl.ds(0, rows), cols]), k_all[:, cols]) * SCALE
        e = jnp.where(mask, jnp.exp(s), 0.0)
        t = jnp.sum(e, axis=-1, keepdims=True)
        prob = (e * (1.0 / t)).astype(BF16)
        att_ref[:, cols] = pick(dot(prob, v_all[:, cols])).astype(BF16)
        totals = jnp.where(lane == 2 * p, t[:rows], totals)
        totals = jnp.where(lane == 2 * p + 1, t[rows:], totals)
    tot_ref[...] = totals
    loads[1].wait()
    hidden_ref[...] = (own + dot(att_ref[...], out_w[...])).astype(BF16)
    up.finish()
    up_cot.finish()
    spread.finish()
    down.drain()
    up.drain()
    up_cot.drain()


def coarse_level(pos, pooled_ref, cg_ref, w_ref, out_w, mixed_ref, grad_ref):
    count, width = pooled_ref.shape[0], w_ref.shape[2]
    normed_b = rms_rows(pooled_ref[...].astype(F32))[0].astype(BF16)
    uq, fq = head_rms(dot(normed_b, w_ref[0]))
    uk, fk = head_rms(dot(normed_b, w_ref[1]))
    qb, kb = uq.astype(BF16), uk.astype(BF16)
    vb = dot(normed_b, w_ref[2]).astype(BF16)
    gb = dot_nt(cg_ref[...], out_w[...]).astype(BF16)
    block = min(count, 256)
    att_p, dq_p, dk_p, dv_p = [], [], [], []
    for p in range(width // PAIR):
        cols = slice(p * PAIR, (p + 1) * PAIR)
        att_b, dq_b, dk, dv = [], [], None, None
        kp, vp = kb[:, cols], vb[:, cols]
        for b in range(count // block):
            rows = slice(b * block, (b + 1) * block)
            qs, gs = both(qb[rows, cols]), both(gb[rows, cols])
            s = dot_nt(qs, kp) * SCALE
            where = iota((2 * block, count), 0) % block + b * block >= iota((2 * block, count), 1)
            e = jnp.where(where, jnp.exp(s), 0.0)
            full = e * (1.0 / jnp.sum(e, axis=-1, keepdims=True))
            prob = full.astype(BF16)
            att = pick(dot(prob, vp)).astype(BF16)
            att_b.append(att)
            att2 = jnp.concatenate([att.astype(F32)] * 2)
            delta = jnp.sum(gs.astype(F32) * att2, axis=-1, keepdims=True)
            ds = (full * (dot_nt(gs, vp) - delta)).astype(BF16)
            dq_b.append(pick(dot(ds, kp)) * SCALE)
            dk_t, dv_t = dot_tn(ds, qs) * SCALE, dot_tn(prob, gs)
            dk = dk_t if dk is None else dk + dk_t
            dv = dv_t if dv is None else dv + dv_t
        att_p.append(jnp.concatenate(att_b))
        dq_p.append(jnp.concatenate(dq_b))
        dk_p.append(dk)
        dv_p.append(dv)
    join = lambda parts: jnp.concatenate(parts, axis=1)
    mixed_ref[...] = dot(join(att_p), out_w[...]).astype(BF16)
    dq = head_back(join(dq_p), uq, fq).astype(BF16)
    dk = head_back(join(dk_p), uk, fk).astype(BF16)
    dv = join(dv_p).astype(BF16)
    total = dot_nt(dq, w_ref[0]) + dot_nt(dk, w_ref[1]) + dot_nt(dv, w_ref[2])
    grad_ref[pl.ds(0, count), :] = total.astype(BF16)
    extra = grad_ref.shape[0] - count
    grad_ref[pl.ds(count, extra), :] = jnp.zeros((extra, D), BF16)


def middle(
    pos, hidden_ref, mixed_in, grad_in, pooled_ref, cg_ref, cot_ref, cot_after, att_ref, tot_ref, out_w,
    output_ref, hg_ref, g_all, delta_ref, stats_ref,
):
    rows = hidden_ref.shape[0]
    outs = rows // POOL
    ahead = cot_after.shape[0]
    far = grad_in.shape[1]
    start = pos[0] * rows
    pooled = pooled_ref[...].astype(F32)
    mixed = jnp.sum(mixed_in[...].astype(F32), axis=0)
    state = (pooled[:outs] + mixed).astype(BF16)
    onto = (iota((rows, outs), 0) // POOL == iota((rows, outs), 1)).astype(F32).astype(BF16)
    output_ref[...] = (hidden_ref[...].astype(F32) + dot(onto, state)).astype(BF16)
    nxt = cot_after[...].astype(F32)
    nxt = jnp.where(start + rows + iota(nxt.shape, 0) < pos[1] * rows, nxt, 0.0)
    cot = jnp.concatenate([cot_ref[...].astype(F32), nxt])
    length = rows + ahead
    near = length // POOL
    groups = (iota((near, length), 1) // POOL == iota((near, length), 0)).astype(F32).astype(BF16)
    cg = jnp.concatenate([dot(groups, cot.astype(BF16)), cg_ref[...].astype(F32)[near:]])
    ng = jnp.sum(grad_in[...].astype(F32), axis=0)
    normed, factor = rms_rows(pooled)
    pg = (cg + row_back(ng, normed, factor)) / POOL
    pg = jnp.where(pos[0] * outs + iota(pg.shape, 0) < pos[1] * outs, pg, 0.0)
    lift = ((iota((length, far), 0) + POOL - 1) // POOL == iota((length, far), 1)).astype(F32).astype(BF16)
    hi, lo = split(pg)
    hidden_grad = cot + dot(lift, hi) + dot(lift, lo)
    hg_ref[...] = hidden_grad[:rows]
    g_all[...] = dot_nt(hidden_grad.astype(BF16), out_w[...]).astype(BF16)
    delta = head_sum(g_all[pl.ds(0, rows), :].astype(F32) * att_ref[...].astype(F32))
    delta_ref[...] = delta
    stats_ref[pl.ds(0, HEADS), :] = tot_ref[...].T[:HEADS]
    stats_ref[pl.ds(HEADS, HEADS), :] = delta.T[:HEADS]


def fine_backward(
    pos, x_ref, next_ref, w_ref, q_own, k_all, v_all, g_all, own_stats, after, tot_ref, delta_ref,
    unit_q, unit_k, scale_q, scale_k, hg_ref, grad_ref,
):
    rows = x_ref.shape[0]
    hops = after.shape[0]
    margin = k_all.shape[0] - rows
    length = g_all.shape[0]
    anchor = pos[0] * rows
    nxt = next_ref[...].astype(F32)
    nxt = jnp.where(anchor + rows + iota(nxt.shape, 0) < pos[1] * rows, nxt, 0.0)
    q_next = head_rms(dot(rms_rows(nxt)[0].astype(BF16), w_ref[0]))[0].astype(BF16)
    q_all = jnp.concatenate([q_own[...], q_next])
    mask = window_mask(rows, margin + rows, anchor)
    mask = jnp.concatenate([mask.astype(F32)] * 2) > 0
    gap = iota((rows, length), 1) - iota((rows, length), 0)
    mask_t = (gap >= 0) & (gap < WINDOW) & (anchor + iota((rows, length), 1) < pos[1] * rows)
    stats = jnp.concatenate([own_stats[...]] + [after[d] for d in range(hops)], axis=1)
    stats = jnp.where(anchor + iota(stats.shape, 1) < pos[1] * rows, stats, 1.0)
    totals, deltas = tot_ref[...], delta_ref[...]
    dq_p, dk_p, dv_p = [], [], []
    for p in range(HEADS // 2):
        cols = pl.ds(p * PAIR, PAIR)
        kp, vp, gp = k_all[:, cols], v_all[:, cols], g_all[:, cols]
        qp = q_all[:, p * PAIR : (p + 1) * PAIR]
        s = dot_nt(both(qp[:rows]), kp) * SCALE
        e = jnp.where(mask, jnp.exp(s), 0.0)
        column = lambda m: jnp.concatenate([m[:, 2 * p : 2 * p + 1], m[:, 2 * p + 1 : 2 * p + 2]])
        ds = e * (1.0 / column(totals)) * (dot_nt(both(gp[:rows]), vp) - column(deltas))
        dq_p.append(pick(dot(ds.astype(BF16), kp)) * SCALE)
        k_own, v_own = kp[margin:], vp[margin:]
        qs, gs = both(qp), both(gp)
        dk = dv = jnp.zeros((rows, PAIR), F32)
        for h in range(2):
            part = slice(h * length, (h + 1) * length)
            st = dot_nt(k_own, qs[part]) * SCALE
            head = 2 * p + h
            pt = jnp.where(mask_t, jnp.exp(st), 0.0) * (1.0 / stats[head : head + 1])
            dst = pt * (dot_nt(v_own, gs[part]) - stats[HEADS + head : HEADS + head + 1])
            dk = dk + dot(dst.astype(BF16), qs[part])
            dv = dv + dot(pt.astype(BF16), gs[part])
        dk_p.append(dk * SCALE)
        dv_p.append(dv)
    join = lambda parts: jnp.concatenate(parts, axis=1)
    dq = head_back(join(dq_p), unit_q[...], scale_q[...]).astype(BF16)
    dk = head_back(join(dk_p), unit_k[...], scale_k[...]).astype(BF16)
    dv = join(dv_p).astype(BF16)
    total = dot_nt(dq, w_ref[0]) + dot_nt(dk, w_ref[1]) + dot_nt(dv, w_ref[2])
    normed, factor = rms_rows(x_ref[...].astype(F32))
    grad_ref[...] = (hg_ref[...] + row_back(total, normed, factor)).astype(BF16)


def per_device(tokens, cotangent, fine_qkv, fine_out, coarse_qkv, coarse_out):
    rows = tokens.shape[0]
    hops = -(-WINDOW // rows)
    outs = rows // POOL
    me, count, subs = place()
    pos = jnp.stack([me, jnp.int32(count)]).astype(jnp.int32)
    far = (hops + 2) * outs
    shape = jax.ShapeDtypeStruct
    dma = pltpu.SemaphoreType.DMA
    fine_w = jnp.transpose(fine_qkv, (1, 0, 2))
    coarse_w = jnp.transpose(coarse_qkv, (1, 0, 2))
    coarse_grad = cotangent.astype(F32).reshape(outs, POOL, D).sum(axis=1).astype(BF16)
    length = (hops + 1) * rows
    flat = lambda a: a.reshape(-1, D)
    q_own, k_all, v_all, unit_q, unit_k, scale_q, scale_k, totals, attended, hidden, cg_all, after, cot_after = comm(
        functools.partial(fine_forward, hops),
        [shape((rows, D), BF16)] + [shape((length, D), BF16)] * 2 + [shape((rows, D), F32)] * 4
        + [shape((rows, 128), F32)] + [shape((rows, D), BF16)] * 2
        + [shape((count, outs, D), BF16)] + [shape((hops, rows, D), BF16)] * 2,
        [pltpu.VMEM((hops, rows, D), BF16), pltpu.VMEM(fine_w.shape, BF16), pltpu.VMEM(fine_out.shape, BF16),
         dma((2,)), dma((3, 2 * hops)), dma((3, hops))] + spread_sems(count, subs),
        0, [VMEM] * 3 + [ANY] * 2, tokens, cotangent, coarse_grad, fine_w, fine_out,
        out_specs=[VMEM] * 13,
    )
    pooled_all = comm(
        second_exchange,
        shape((count, outs, D), BF16),
        [pltpu.VMEM((POOL, D), BF16), pltpu.VMEM((outs, D), BF16), dma, dma] + spread_sems(count, subs),
        1, [VMEM], hidden, out_specs=VMEM,
    )
    pooled_all, cg_all = flat(pooled_all), flat(cg_all)
    mixed_all, grad_all = local_call(
        coarse_level,
        [shape((count * outs, D), BF16), shape((count * outs + far, D), BF16)],
        pos, pooled_all, cg_all, coarse_w, coarse_out,
    )
    mixed_in, grad_in = comm(
        functools.partial(third_exchange, far),
        (shape((subs, outs, D), BF16), shape((subs, far, D), BF16)),
        [dma((2 * subs,)), dma((2 * subs,)), dma((2,))],
        2, [VMEM, VMEM], mixed_all, grad_all,
    )
    tail = lambda a: lax.dynamic_slice_in_dim(jnp.pad(a, ((0, far), (0, 0))), me * outs, far)
    output, hidden_grad, g_all, delta, stats = local_call(
        middle,
        [shape((rows, D), BF16), shape((rows, D), F32), shape((length, D), BF16),
         shape((rows, 128), F32), shape((2 * HEADS, rows), F32)],
        pos, hidden, mixed_in, grad_in, tail(pooled_all), tail(cg_all), cotangent, flat(cot_after),
        attended, totals, fine_out,
    )
    stats_after = comm(
        functools.partial(fourth_exchange, hops),
        shape((hops, 2 * HEADS, rows), F32),
        [dma((hops,)), dma((hops,))],
        3, [VMEM], stats,
    )
    grad_tokens = local_call(
        fine_backward, shape((rows, D), BF16),
        pos, tokens, flat(after), fine_w, q_own, k_all, v_all, g_all, stats, stats_after, totals, delta,
        unit_q, unit_k, scale_q, scale_k, hidden_grad,
    )
    return (output, grad_tokens)


def solution(mesh):
    placed = (
        P(("seq", "sub"), None),
        P(("seq", "sub"), None),
        P(),
        P(),
        P(None, None, "sub"),
        P("sub", None),
    )
    return jax.shard_map(
        per_device,
        mesh=mesh,
        in_specs=placed,
        out_specs=(P(("seq", "sub"), None), P(("seq", "sub"), None)),
        check_vma=False,
    )
```
